32 devices in a mesh: dp: 8 (over z, y), mp: 4 (over x, core).
Axes of the slice: x: 2, y: 2, z: 4, core: 2. Of those that a mesh axis runs over, the one named last changes fastest.
Arguments:
- features: bfloat16 [3, 512, 16384], P(None, 'mp', 'dp'), may hold values from -6 to 6
- weights: bfloat16 [11, 512, 512], P(None, 'mp'), may hold values from -0.25 to 0.25
- sample_owner: int32 [3, 16384, 1], P(None, 'dp'), may hold values from 0 to 7; in each aligned block of 2048 rows (0 to 2047, 2048 to 4095, ..., all dimensions but the last counted through in order) at most 512 rows name the same one
- sample_row: int32 [3, 16384], P(None, 'dp'), may hold values from 0 to 2047
- edge_src: int32 [8, 16384], P(None, 'dp'), may hold values from 0 to 2047
- edge_dst: int32 [8, 16384], P(None, 'dp'), may hold values from 0 to 127
- edge_count: int32 [8, 8], P(None, 'dp'), may hold values from 128 to 2048
Outputs:
- updated: bfloat16 [3, 512, 1024], P(None, 'mp', 'dp')
The draws below stay inside these ranges and needn't reach their ends.
Inputs may be any that keep to these rules, and one draw needn't show every extreme that they name: `sample_owner`: among the 2048 entries of one node type in one block no owner appears more than 512 times; some owner appears exactly 512 times in some blocks.
All inputs are finite; a program needn't handle non-finite values.
Results may differ from the reference program's by a relative error of at most 0.0064.
Values may be sent and summed in bfloat16 or wider, within the bound.
A program may use at most 64 MiB of HBM per device.

```python
import math
import jax
import jax.numpy as jnp
import numpy as np
from jax import lax

D = 512
RELS = 8
TYPES = 3
MATS = 11
ROWS_DEV = 2048
SAMP = 2048
SEEDS = 128
EDGES = 2048
CAP = 512
TABLE_ROWS = 16384
SAMPLES = 16384
EDGES_ALL = 16384
N_DP = 8


def plant(values, stream_key, smallest, high):
    extent = values.shape
    spot = [jax.random.randint(jax.random.fold_in(stream_key, axis), (), 0, extent[axis]) for axis in range(len(extent))]
    values = values.at[tuple(spot)].set(smallest)
    longest = extent.index(max(extent))
    spot[longest] = (spot[longest] + 1) % extent[longest]
    return values.at[tuple(spot)].set(high)


def level_of(rng, shape, cuts, low, largest):
    loudness = 1.0
    for position, shards_of in cuts:
        draws = jax.random.uniform(jax.random.fold_in(jax.random.fold_in(rng, 6), position), (shards_of,), jnp.float32, low / len(cuts), largest / len(cuts))
        loudness = loudness * jnp.repeat(jnp.exp(draws), shape[position] // shards_of).reshape((-1,) + (1,) * (len(shape) - 1 - position))
    return loudness


def assign_block(own_key, own, number, rows, count, top, limit, lean):
    sequence = jax.random.permutation(own_key, count)
    heavy_load, common = portions_of(count, rows * top, limit, lean, True), portions_of(count, rows * top, limit, lean, False)
    places = jnp.arange(count)

    def named(tallies, rotation):
        used = int((tallies > 0).sum())
        fixed = max(1, used // 4)
        passed = fixed + (places - fixed + rotation * (used - fixed)) % max(1, count - fixed)
        return jnp.zeros((count,), jnp.int32).at[sequence[jnp.where(places < fixed, places, passed)]].set(jnp.asarray(tallies, jnp.int32))

    tallies = jnp.where(number % 4 == 0, named(heavy_load, number // 4), named(common, number - number // 4 - 1))
    mixed = jax.random.permutation(jax.random.fold_in(own, 3), count)
    source_of, sink = mixed[0:count // 2 * 2:2], mixed[1:count // 2 * 2:2]
    margin = jnp.minimum(tallies[source_of] - 1, limit - tallies[sink]) // 2
    margin = jnp.where((source_of == sequence[0]) | (sink == sequence[0]) | (tallies[sink] == 0), 0, jnp.maximum(margin, 0))
    passed = jax.random.randint(jax.random.fold_in(own, 4), (count // 2,), 0, 1 << 20) % (margin + 1)
    tallies = tallies.at[source_of].add(-passed).at[sink].add(passed)
    labels = jnp.searchsorted(jnp.cumsum(tallies), jnp.arange(rows * top), side="right").astype(jnp.int32)
    listing = labels.reshape(top, rows).T
    listing = listing[jax.random.permutation(jax.random.fold_in(own, 1), rows)]
    rotation = jax.random.randint(jax.random.fold_in(own, 2), (rows, 1), 0, top)
    return jnp.take_along_axis(listing, (jnp.arange(top)[None, :] + rotation) % top, axis=1)


def portions_of(count, total, limit, skew, full):
    loads = [(1 << 20) // math.isqrt(standing ** skew) + 1 for standing in range(1, count + 1)]
    largest = limit if full else min(limit, max(-(-total // count), total * loads[0] // sum(loads)))
    least = 1 if total - largest >= count - 1 else 0
    given, rest = [largest] + [least] * (count - 1), total - largest - least * (count - 1)
    while rest > 0:
        free = [i for i in range(1, count) if given[i] < largest] or [i for i in range(1, count) if given[i] < limit]
        whole, left = sum([loads[i] for i in free]), rest
        for i in free:
            more = min(limit - given[i], max(1, left * loads[i] // whole), rest)
            given[i] = given[i] + more
            rest = rest - more
    return np.array(given)


def normal_values(key, dims, width, most, split=(), kind=jnp.bfloat16):
    drawn = jax.random.normal(key, dims, jnp.float32) * width
    if len(split) > 0:
        drawn = level_of(key, dims, split, -0.22, 0.18) * drawn
    return jnp.clip(drawn, min=-most, max=most).astype(kind)


def setup_inputs(seed: int = 0) -> dict:
    arg_keys = jax.random.split(jax.random.key(seed), 8)
    features = normal_values(arg_keys[0], (TYPES, D, TABLE_ROWS), 1.0, 6.0, ((1, 4), (2, 8)))
    weights = normal_values(arg_keys[1], (MATS, D, D), D ** -0.5, 0.25, ((1, 4),))
    sample_owner_keys = jax.random.split(jax.random.fold_in(arg_keys[2], 1), TYPES * SAMPLES // SAMP)
    sample_owner_turns = jax.random.permutation(jax.random.fold_in(arg_keys[2], 3), TYPES * SAMPLES // SAMP)
    sample_owner = jax.vmap(lambda own, number: assign_block(jax.random.fold_in(arg_keys[2], 2), own, number, SAMP, N_DP, 1, CAP, 2))(sample_owner_keys, sample_owner_turns).reshape((TYPES, SAMPLES, 1))
    sample_row = plant(jax.random.randint(arg_keys[3], (TYPES, SAMPLES), 0, ROWS_DEV), jax.random.fold_in(arg_keys[3], 1), 0, ROWS_DEV - 1).astype(jnp.int32)
    edge_src = plant(jax.random.randint(arg_keys[4], (RELS, EDGES_ALL), 0, SAMP), jax.random.fold_in(arg_keys[4], 1), 0, SAMP - 1).astype(jnp.int32)
    edge_dst = plant(jax.random.randint(arg_keys[5], (RELS, EDGES_ALL), 0, SEEDS), jax.random.fold_in(arg_keys[5], 1), 0, SEEDS - 1).astype(jnp.int32)
    edge_count = plant(jax.random.randint(arg_keys[6], (RELS, N_DP), EDGES // 16, EDGES + 1), jax.random.fold_in(arg_keys[6], 1), EDGES // 16, EDGES).astype(jnp.int32)
    return {"features": features, "weights": weights, "sample_owner": sample_owner, "sample_row": sample_row, "edge_src": edge_src, "edge_dst": edge_dst, "edge_count": edge_count}


RELATION_SOURCE = (0, 1, 0, 1, 2, 0, 2, 1)
RELATION_TARGET = (1, 0, 0, 2, 1, 2, 0, 1)


def reference(features, weights, sample_owner, sample_row, edge_src, edge_dst, edge_count):
    row_index = (sample_owner[:, :, 0] * ROWS_DEV + sample_row).astype(jnp.int32)
    block_index = row_index.reshape(TYPES, N_DP, SAMP).transpose(1, 0, 2)
    block_src = edge_src.reshape(RELS, N_DP, EDGES).transpose(1, 0, 2)
    block_dst = edge_dst.reshape(RELS, N_DP, EDGES).transpose(1, 0, 2)
    block_count = edge_count.transpose(1, 0)

    def one_block(inputs):
        index_here, src_here, dst_here, count_here = inputs
        fetched = [jnp.take(features[node_kind], index_here[node_kind], axis=1).T for node_kind in range(TYPES)]
        typed = [jnp.dot(fetched[node_kind][:SEEDS], weights[RELS + node_kind], preferred_element_type=jnp.float32) for node_kind in range(TYPES)]
        slot_ids = jnp.arange(EDGES, dtype=jnp.int32)
        for relation in range(RELS):
            live_edge = (slot_ids < count_here[relation]).astype(jnp.float32)
            sources = jnp.take(fetched[RELATION_SOURCE[relation]], src_here[relation], axis=0).astype(jnp.float32)
            summed = jax.ops.segment_sum(sources * live_edge[:, None], dst_here[relation], num_segments=SEEDS)
            degree = jax.ops.segment_sum(live_edge, dst_here[relation], num_segments=SEEDS)
            message = (summed / jnp.maximum(degree, 1.0)[:, None]).astype(jnp.bfloat16)
            target = RELATION_TARGET[relation]
            typed[target] = typed[target] + jnp.dot(message, weights[relation], preferred_element_type=jnp.float32)
        return jnp.stack([jax.nn.relu(value).astype(jnp.bfloat16) for value in typed])

    result = lax.map(one_block, (block_index, block_src, block_dst, block_count))
    return result.transpose(1, 3, 0, 2).reshape(TYPES, result.shape[3], N_DP * SEEDS)
```

```python
import functools

import jax
import jax.numpy as jnp
from jax import lax
from jax.experimental import pallas as pl
from jax.experimental.pallas import tpu as pltpu
from jax.sharding import PartitionSpec as P

SEEDS = 128
RELATION_SOURCE = (0, 1, 0, 1, 2, 0, 2, 1)
MATRIX_TARGET = (1, 0, 0, 2, 1, 2, 0, 1, 0, 1, 2)
RELS = len(RELATION_SOURCE)
KINDS = 3
MATS = RELS + KINDS
SLOTS = tuple(
    tuple([r for r in range(RELS) if RELATION_SOURCE[r] == k] + [RELS + k]) for k in range(KINDS)
)
ORDER = tuple(m for group in SLOTS for m in group)
STARTS = tuple(sum(len(group) for group in SLOTS[:k]) for k in range(KINDS))
PLACE = tuple(ORDER.index(m) for m in range(MATS))
CORES = 2
SHARE = RELS // CORES
STEP = 256
LANES = 128
MESH = pl.DeviceIdType.MESH
NT = (((1,), (1,)), ((), ()))


def log2(n):
    return n.bit_length() - 1


def kernel(groups, shares, features_in, weights_in, owner, row, src, dst, count, out,
           feats, weights, iota, req_send, req_recv, info_send, info_recv, table,
           lidx, ridx, picked, adj, message, hold, xsend, xrecv, zsend, zrecv,
           in_sem, fx_ss, fx_rs, req_ss, req_rs, info_ss, info_rs, x_ss, x_rs, z_ss, z_rs):
    kinds, _, feat, rows = feats.shape
    both = CORES * feat
    sampled = row.shape[1]
    edge_total = src.shape[1]
    cap = req_send.shape[2] - SEEDS
    low = min(512, rows)
    high = rows // low
    lo_n = min(STEP, cap)
    hi_n = cap // lo_n
    items = groups // CORES
    planes = shares // CORES
    half = hold.shape[3]
    quarter = half // CORES
    g = lax.axis_index("dp")
    m = lax.axis_index("mp")
    core = lax.rem(m, CORES)
    plane = m // CORES
    f32, bf16, i32 = jnp.float32, jnp.bfloat16, jnp.int32
    one, zero = jnp.ones((), bf16), jnp.zeros((), bf16)

    def at(group, mp):
        return {"dp": group, "mp": mp}

    def remote(source, target, ss, rs, group, mp):
        return pltpu.make_async_remote_copy(source, target, ss, rs, device_id=at(group, mp), device_id_type=MESH)

    def hits(index, size):
        n = index.shape[1]
        return jnp.where(iota[:size, :n] == index.astype(f32).astype(bf16), one, zero)

    mate = m - core + lax.rem(core + 1, CORES)
    loads, swaps = [], []
    for k in range(kinds):
        loads.append(pltpu.make_async_copy(features_in.at[k], feats.at[k, core], in_sem.at[k]))
        swaps.append(remote(features_in.at[k], feats.at[k, core], fx_ss.at[k], fx_rs.at[k], g, mate))
    loads.append(pltpu.make_async_copy(weights_in, weights.at[core], in_sem.at[kinds]))
    swaps.append(remote(weights_in, weights.at[core], fx_ss.at[kinds], fx_rs.at[kinds], g, mate))
    for copy in loads:
        copy.start()

    barrier = pltpu.get_barrier_semaphore()
    pl.semaphore_signal(barrier, inc=1, device_id=at(g, mate), device_id_type=MESH)
    for d in range(1, groups):
        for c in range(CORES):
            pl.semaphore_signal(barrier, inc=1, device_id=at(g ^ d, plane * CORES + c), device_id_type=MESH)
    for e in range(1, planes):
        pl.semaphore_signal(
            barrier, inc=1, device_id=at(g, lax.rem(plane + e, planes) * CORES + core), device_id_type=MESH)

    iota[...] = lax.broadcasted_iota(i32, iota.shape, 0).astype(f32).astype(bf16)
    tri = (lax.broadcasted_iota(i32, (STEP, STEP), 0) <= lax.broadcasted_iota(i32, (STEP, STEP), 1))
    tri = jnp.where(tri, 1.0, 0.0).astype(bf16)
    hot = jnp.concatenate([
        jnp.where(lax.broadcasted_iota(i32, (groups, sampled), 0) == owner[k], 1.0, 0.0)
        for k in range(kinds)], axis=0)
    lines = kinds * groups
    pieces = [hot[:, base:base + STEP] for base in range(0, sampled, STEP)]
    upto = jnp.dot(jnp.concatenate(pieces, axis=0).astype(bf16), tri, preferred_element_type=f32)
    carry = jnp.zeros((lines, 1), f32)
    ranks = []
    for n, piece in enumerate(pieces):
        here = upto[n * lines:(n + 1) * lines]
        ranks.append((here + (carry - 1.0)) * piece)
        carry = carry + here[:, STEP - 1:]
    ranks = jnp.concatenate(ranks, axis=1)

    pl.semaphore_wait(barrier, CORES * (groups - 1) + planes)
    for copy in swaps:
        copy.start()

    blocks = sampled // LANES
    parts = cap // LANES
    for k in range(kinds):
        mine = hot[k * groups:(k + 1) * groups]
        rank = jnp.sum(ranks[k * groups:(k + 1) * groups], axis=0, keepdims=True).astype(i32)
        place = owner[k] * cap + rank
        coarse = (place >> 8).astype(f32)
        fine = (place & 255).astype(f32)
        table[k] = jnp.concatenate(
            [part[:, b * LANES:(b + 1) * LANES] for part in (coarse, fine) for b in range(blocks)], axis=0).astype(bf16)
        wanted = row[k:k + 1, :]
        tall = mine * (wanted >> 8).astype(f32)
        wide = mine * (wanted & 255).astype(f32)
        bank = rank >> log2(LANES)
        stack = jnp.concatenate(
            [jnp.where(bank == h, part, 0.0) for part in (tall, wide) for h in range(parts)], axis=0).astype(bf16)
        listed = lax.dot_general(stack, hits(rank & (LANES - 1), LANES), NT, preferred_element_type=f32)
        listed = (listed[:parts * groups] * 256.0 + listed[parts * groups:]).astype(i32)
        seeds = jnp.where(mine[:, :SEEDS] > 0.0, rank[:, :SEEDS], -1)
        for o in range(groups):
            for h in range(parts):
                req_send[o, k:k + 1, h * LANES:(h + 1) * LANES] = listed[h * groups + o:h * groups + o + 1]
            req_send[o, k:k + 1, cap:] = seeds[o:o + 1]

    requests = []
    def order(i):
        return 0 if i == 0 else 1 if i == items - 1 else i + 1

    def request_copy(t):
        to = g ^ (CORES * t + core)
        return remote(req_send.at[to], req_recv.at[t], req_ss.at[t], req_rs.at[t], to, m)

    for i in range(items):
        t = order(i)
        if t == 0:
            @pl.when(core > 0)
            def _():
                request_copy(0).start()

            @pl.when(core == 0)
            def _():
                req_recv[0] = req_send[g]
        else:
            request_copy(t).start()

    slots = lax.broadcasted_iota(i32, (1, edge_total), 1)
    banks = lax.broadcasted_iota(i32, (blocks, edge_total), 0)
    ones8 = jnp.ones((8, LANES), bf16)
    for j in range(SHARE):
        r = core * SHARE + j
        kind = RELATION_SOURCE[j] + core * (RELATION_SOURCE[SHARE + j] - RELATION_SOURCE[j])
        wanted = src[pl.ds(r, 1), :]
        found = jnp.dot(table[kind], hits(wanted & (LANES - 1), LANES), preferred_element_type=f32)
        found = found[:blocks] * 256.0 + found[blocks:]
        found = jnp.where(banks == (wanted >> log2(LANES)), found, 0.0)
        place = jnp.sum(found, axis=0, keepdims=True).astype(i32)
        live = slots < count[0, r]
        ends = dst[pl.ds(r, 1), :]
        info_send[j:j + 1, :edge_total] = jnp.where(live, place * SEEDS + ends, -1)
        marks = hits(jnp.where(live, ends, -1), SEEDS)
        tally = marks[:, :LANES]
        for base in range(LANES, edge_total, LANES):
            tally = tally + marks[:, base:base + LANES]
        tally = lax.dot_general(ones8, tally, NT, preferred_element_type=f32)
        info_send[j:j + 1, edge_total:] = tally[:1].astype(i32)

    def info_copy(d):
        return remote(info_send, info_recv.at[d // CORES, core], info_ss.at[d], info_rs.at[d // CORES, core],
                      g ^ d, plane * CORES + d % CORES)

    for i in range(items):
        for c in reversed(range(CORES)):
            d = CORES * order(i) + c
            if d == 0:
                @pl.when(core > 0)
                def _():
                    info_copy(0).start()

                @pl.when(core == 0)
                def _():
                    info_recv[0, 0] = info_send[...]
            else:
                info_copy(d).start()

    def info_wait(t, c):
        remote(info_send, info_recv.at[t, c], info_ss.at[0], info_rs.at[t, c], g, mate).wait_recv()

    for copy in loads:
        copy.wait()
    for copy in swaps:
        copy.wait()

    def x_copy(i, e, t):
        to = lax.rem(plane + e, planes) * CORES + core
        return remote(xsend.at[i, e, t], xrecv.at[i, e, t], x_ss.at[i, e, t], x_rs.at[i, e, t], g, to)

    def z_copy(i, d, c, t):
        return remote(zsend.at[i, c, t], zrecv.at[d, t], z_ss.at[i, c, t], z_rs.at[d, t],
                      g ^ d, plane * CORES + c)

    def spot(i):
        return jnp.where(i == 0, 0, jnp.where(i == items - 1, 1, i + 1))

    def forward(i, t):
        d = CORES * spot(i) + core
        total = hold[i, t]
        for e in range(1, planes):
            x_copy(i, e, t).wait_recv()
            total = total + xrecv[i, e, t].astype(f32)
        total = total.astype(bf16)
        for c in range(CORES):
            zsend[i, c, t] = total[:, c * quarter:(c + 1) * quarter]
        for c in range(1, CORES):
            z_copy(i, d, c, t).start()

        @pl.when(d > 0)
        def _():
            z_copy(i, d, 0, t).start()

        @pl.when(d == 0)
        def _():
            zrecv[0, t] = total[:, :quarter]

    def build(place, ref_l, ref_r, n, width):
        left = hits(ref_l[pl.ds(n, 1), :width], lo_n) if width <= STEP else jnp.concatenate(
            [hits(ref_l[pl.ds(n, 1), base:base + STEP], lo_n) for base in range(0, width, STEP)], axis=1)
        right = hits(ref_r[pl.ds(n, 1), :width], hi_n * SEEDS) if width <= STEP else jnp.concatenate(
            [hits(ref_r[pl.ds(n, 1), base:base + STEP], hi_n * SEEDS) for base in range(0, width, STEP)], axis=1)
        counts = lax.dot_general(right, left, NT, preferred_element_type=f32).astype(bf16)
        for h in range(hi_n):
            adj[place, :, h * lo_n:(h + 1) * lo_n] = counts[h * SEEDS:(h + 1) * SEEDS]

    def item(i, _):
        t = spot(i)
        d = CORES * t + core

        @pl.when(d > 0)
        def _():
            request_copy(t).wait_recv()
            info_wait(t, 0)

        info_wait(t, 1)
        for k in range(kinds):
            wanted = req_recv[t, k:k + 1, :cap]
            table_k = feats[k].reshape(both, rows)
            table_k = jnp.concatenate([table_k[:, h * low:(h + 1) * low] for h in range(high)], axis=0)
            fine = wanted & (low - 1)
            choice = jnp.concatenate(
                [hits(jnp.where((fine >= base) & (fine < base + STEP), fine - base, -1), STEP)
                 for base in range(0, low, STEP)], axis=0)
            found = jnp.dot(table_k, choice, preferred_element_type=f32)
            bank = wanted >> log2(low)
            chosen = found[:both]
            for h in range(1, high):
                chosen = jnp.where(bank == h, found[h * both:(h + 1) * both], chosen)
            picked[k] = chosen.astype(bf16)

        for c in range(CORES):
            packed = info_recv[t, c, :, :edge_total] - g * (cap * SEEDS)
            ok = (packed >= 0) & (packed < cap * SEEDS)
            slot = packed >> log2(SEEDS)
            lidx[c * SHARE:(c + 1) * SHARE, :] = (slot & (lo_n - 1)).astype(f32)
            ridx[c * SHARE:(c + 1) * SHARE, :] = jnp.where(
                ok, (slot >> log2(lo_n)) * SEEDS + (packed & (SEEDS - 1)), -1).astype(f32)
        slot = req_recv[t, :, cap:]
        lidx[RELS:RELS + kinds, :SEEDS] = (slot & (lo_n - 1)).astype(f32)
        ridx[RELS:RELS + kinds, :SEEDS] = jnp.where(
            slot >= 0, (slot >> log2(lo_n)) * SEEDS + lax.broadcasted_iota(i32, slot.shape, 1), -1).astype(f32)

        def relation(r, _):
            build(r, lidx, ridx, r, edge_total)
            return 0

        lax.fori_loop(0, RELS, relation, 0)
        for k in range(kinds):
            build(RELS + k, lidx, ridx, RELS + k, SEEDS)

        @pl.when(i > 0)
        def _():
            for n in range(kinds):
                forward(i - 1, n)

        degree = jnp.concatenate([info_recv[t, c, :, edge_total:] for c in range(CORES)], axis=0)
        inverse = (1.0 / jnp.maximum(degree.astype(f32), 1.0)).T
        for k in range(kinds):
            group = SLOTS[k]
            counts = jnp.concatenate([adj[n] for n in group], axis=0)
            summed = lax.dot_general(counts, picked[k], NT, preferred_element_type=f32)
            for n, matrix in enumerate(group):
                value = summed[n * SEEDS:(n + 1) * SEEDS]
                if matrix < RELS:
                    value = value * inverse[:, matrix:matrix + 1]
                message[matrix] = value.astype(bf16)
        for n in range(kinds):
            group = [matrix for matrix in range(MATS) if MATRIX_TARGET[matrix] == n]
            left = jnp.concatenate([message[matrix] for matrix in group], axis=1)
            right = jnp.concatenate([weights[c, matrix] for matrix in group for c in range(CORES)], axis=0)
            typed = jnp.dot(left, right, preferred_element_type=f32)
            for p in range(planes):
                piece = typed[:, p * half:(p + 1) * half]

                @pl.when(plane == p)
                def _(piece=piece, n=n):
                    hold[i, n] = piece

                @pl.when(plane != p)
                def _(piece=piece, n=n, p=p):
                    xsend[i, lax.rem(p - plane + planes, planes), n] = piece.astype(bf16)
            for e in range(1, planes):
                x_copy(i, e, n).start()
        return 0

    lax.fori_loop(0, items, item, 0)
    for n in range(kinds):
        forward(items - 1, n)

    for n in range(kinds):
        total = jnp.zeros((SEEDS, quarter), f32)
        for i in range(items):
            for c in reversed(range(CORES)):
                d = CORES * order(i) + c
                if d == 0:
                    @pl.when(core > 0)
                    def _():
                        z_copy(0, 0, 0, n).wait_recv()
                else:
                    z_copy(0, d, 0, n).wait_recv()
                total = total + zrecv[d, n].astype(f32)
        out[n] = jnp.maximum(total, 0.0).T.astype(bf16)

    for t in range(items):
        if t == 0:
            @pl.when(core > 0)
            def _():
                request_copy(0).wait_send()
                info_copy(0).wait_send()
        else:
            request_copy(t).wait_send()
            info_copy(CORES * t).wait_send()
        for c in range(1, CORES):
            info_copy(CORES * t + c).wait_send()
        for n in range(kinds):
            for e in range(1, planes):
                x_copy(t, e, n).wait_send()
            d = CORES * spot(t) + core
            for c in range(1, CORES):
                z_copy(t, d, c, n).wait_send()

            @pl.when(d > 0)
            def _():
                z_copy(t, d, 0, n).wait_send()


def per_device(features, weights, sample_owner, sample_row, edge_src, edge_dst, edge_count):
    groups, shares = lax.axis_size("dp"), lax.axis_size("mp")
    kinds, feat, rows = features.shape
    sampled, edge_total = sample_row.shape[1], edge_src.shape[1]
    cap = 2 * sampled // groups
    items, planes = groups // CORES, shares // CORES
    width = weights.shape[2]
    half, quarter = width // planes, width // shares
    bf16, f32, i32 = jnp.bfloat16, jnp.float32, jnp.int32
    vmem = pl.BlockSpec(memory_space=pltpu.VMEM)
    any_space = pl.BlockSpec(memory_space=pl.ANY)
    dma = pltpu.SemaphoreType.DMA
    return pl.pallas_call(
        functools.partial(kernel, groups, shares),
        out_shape=jax.ShapeDtypeStruct((kinds, quarter, SEEDS), bf16),
        in_specs=[any_space] * 2 + [vmem] * 4 + [pl.BlockSpec(memory_space=pltpu.SMEM)],
        out_specs=vmem,
        scratch_shapes=[
            pltpu.VMEM((kinds, CORES, feat, rows), bf16),
            pltpu.VMEM((CORES, MATS, feat, width), bf16),
            pltpu.VMEM((STEP, max(sampled, edge_total)), bf16),
            pltpu.VMEM((groups, kinds, cap + SEEDS), i32),
            pltpu.VMEM((items, kinds, cap + SEEDS), i32),
            pltpu.VMEM((SHARE, edge_total + SEEDS), i32),
            pltpu.VMEM((items, CORES, SHARE, edge_total + SEEDS), i32),
            pltpu.VMEM((kinds, 2 * sampled // LANES, LANES), bf16),
            pltpu.VMEM((16, edge_total), f32),
            pltpu.VMEM((16, edge_total), f32),
            pltpu.VMEM((kinds, CORES * feat, cap), bf16),
            pltpu.VMEM((MATS, SEEDS, cap), bf16),
            pltpu.VMEM((MATS, SEEDS, CORES * feat), bf16),
            pltpu.VMEM((items, kinds, SEEDS, half), f32),
            pltpu.VMEM((items, planes, kinds, SEEDS, half), bf16),
            pltpu.VMEM((items, planes, kinds, SEEDS, half), bf16),
            pltpu.VMEM((items, CORES, kinds, SEEDS, quarter), bf16),
            pltpu.VMEM((groups, kinds, SEEDS, quarter), bf16),
            dma((kinds + 1,)), dma((kinds + 1,)), dma((kinds + 1,)),
            dma((items,)), dma((items,)),
            dma((groups,)), dma((items, CORES)),
            dma((items, planes, kinds)), dma((items, planes, kinds)),
            dma((items, CORES, kinds)), dma((groups, kinds)),
        ],
        compiler_params=pltpu.CompilerParams(
            collective_id=0, has_side_effects=True, vmem_limit_bytes=60 * 1024 * 1024),
    )(features, weights, sample_owner.transpose(0, 2, 1), sample_row, edge_src, edge_dst, edge_count.T)


def solution(mesh):
    return jax.shard_map(
        per_device,
        mesh=mesh,
        in_specs=(
            P(None, "mp", "dp"),
            P(None, "mp", None),
            P(None, "dp", None),
            P(None, "dp"),
            P(None, "dp"),
            P(None, "dp"),
            P(None, "dp"),
        ),
        out_specs=P(None, "mp", "dp"),
        check_vma=False,
    )
```

```python
import functools

import jax
import jax.numpy as jnp
from jax import lax
from jax.experimental import pallas as pl
from jax.experimental.pallas import tpu as pltpu
from jax.sharding import PartitionSpec as P

SEEDS = 128
RELATION_SOURCE = (0, 1, 0, 1, 2, 0, 2, 1)
MATRIX_TARGET = (1, 0, 0, 2, 1, 2, 0, 1, 0, 1, 2)
RELS = len(RELATION_SOURCE)
KINDS = 3
MATS = RELS + KINDS
SLOTS = tuple(
    tuple([r for r in range(RELS) if RELATION_SOURCE[r] == k] + [RELS + k]) for k in range(KINDS)
)
ORDER = tuple(m for group in SLOTS for m in group)
STARTS = tuple(sum(len(group) for group in SLOTS[:k]) for k in range(KINDS))
PLACE = tuple(ORDER.index(m) for m in range(MATS))
CORES = 2
WAYS = 2
SHARE = RELS // CORES
STEP = 256
LANES = 128
MESH = pl.DeviceIdType.MESH
NT = (((1,), (1,)), ((), ()))


def log2(n):
    return n.bit_length() - 1


def kernel(groups, shares, features_in, weights_in, owner, row, src, dst, count, out,
           feats, weights, iota, req_send, req_recv, info_send, info_recv, table,
           lidx, ridx, picked, adj, xsend, xrecv, yrecv, zsend, zrecv,
           in_sem, fx_ss, fx_rs, req_ss, req_rs, info_ss, info_rs, x_ss, x_rs, y_ss, y_rs, z_ss, z_rs, own_ss, own_rs):
    kinds, _, feat, rows = feats.shape
    both = CORES * feat
    sampled = row.shape[1]
    edge_total = src.shape[1]
    cap = req_send.shape[2] - SEEDS
    low = min(512, rows)
    high = rows // low
    lo_n = min(STEP, cap)
    hi_n = cap // lo_n
    items = groups // CORES
    planes = shares // CORES
    quarter = xsend.shape[6]
    span = SEEDS // WAYS
    half = CORES * quarter
    g = lax.axis_index("dp")
    m = lax.axis_index("mp")
    core = lax.rem(m, CORES)
    plane = m // CORES
    f32, bf16, i32 = jnp.float32, jnp.bfloat16, jnp.int32
    one, zero = jnp.ones((), bf16), jnp.zeros((), bf16)

    def at(group, mp):
        return {"dp": group, "mp": mp}

    def remote(source, target, ss, rs, group, mp):
        return pltpu.make_async_remote_copy(source, target, ss, rs, device_id=at(group, mp), device_id_type=MESH)

    def hits(index, size):
        n = index.shape[1]
        return jnp.where(iota[:size, :n] == index.astype(f32).astype(bf16), one, zero)

    mate = m - core + lax.rem(core + 1, CORES)
    loads, swaps = [], []
    for k in range(kinds):
        loads.append(pltpu.make_async_copy(features_in.at[k], feats.at[k, core], in_sem.at[k]))
        swaps.append(remote(features_in.at[k], feats.at[k, core], fx_ss.at[k], fx_rs.at[k], g, mate))
    loads.append(pltpu.make_async_copy(weights_in, weights.at[core], in_sem.at[kinds]))
    swaps.append(remote(weights_in, weights.at[core], fx_ss.at[kinds], fx_rs.at[kinds], g, mate))
    for copy in loads:
        copy.start()

    barrier = pltpu.get_barrier_semaphore()
    pl.semaphore_signal(barrier, inc=1, device_id=at(g, mate), device_id_type=MESH)
    for d in range(1, groups):
        for c in range(CORES):
            pl.semaphore_signal(barrier, inc=1, device_id=at(g ^ d, plane * CORES + c), device_id_type=MESH)
    for e in range(1, planes):
        pl.semaphore_signal(
            barrier, inc=1, device_id=at(g, lax.rem(plane + e, planes) * CORES + core), device_id_type=MESH)

    iota[...] = lax.broadcasted_iota(i32, iota.shape, 0).astype(f32).astype(bf16)
    tri = (lax.broadcasted_iota(i32, (STEP, STEP), 0) <= lax.broadcasted_iota(i32, (STEP, STEP), 1))
    tri = jnp.where(tri, 1.0, 0.0).astype(bf16)
    hot = jnp.concatenate([
        jnp.where(lax.broadcasted_iota(i32, (groups, sampled), 0) == owner[k], 1.0, 0.0)
        for k in range(kinds)], axis=0)
    lines = kinds * groups
    pieces = [hot[:, base:base + STEP] for base in range(0, sampled, STEP)]
    upto = jnp.dot(jnp.concatenate(pieces, axis=0).astype(bf16), tri, preferred_element_type=f32)
    carry = jnp.zeros((lines, 1), f32)
    ranks = []
    for n, piece in enumerate(pieces):
        here = upto[n * lines:(n + 1) * lines]
        ranks.append((here + (carry - 1.0)) * piece)
        carry = carry + here[:, STEP - 1:]
    ranks = jnp.concatenate(ranks, axis=1)

    pl.semaphore_wait(barrier, CORES * (groups - 1) + planes)
    for copy in swaps:
        copy.start()

    blocks = sampled // LANES
    parts = cap // LANES
    for k in range(kinds):
        mine = hot[k * groups:(k + 1) * groups]
        rank = jnp.sum(ranks[k * groups:(k + 1) * groups], axis=0, keepdims=True).astype(i32)
        place = owner[k] * cap + rank
        coarse = (place >> 8).astype(f32)
        fine = (place & 255).astype(f32)
        table[k] = jnp.concatenate(
            [part[:, b * LANES:(b + 1) * LANES] for part in (coarse, fine) for b in range(blocks)], axis=0).astype(bf16)
        wanted = row[k:k + 1, :]
        tall = mine * (wanted >> 8).astype(f32)
        wide = mine * (wanted & 255).astype(f32)
        bank = rank >> log2(LANES)
        stack = jnp.concatenate(
            [jnp.where(bank == h, part, 0.0) for part in (tall, wide) for h in range(parts)], axis=0).astype(bf16)
        listed = lax.dot_general(stack, hits(rank & (LANES - 1), LANES), NT, preferred_element_type=f32)
        listed = (listed[:parts * groups] * 256.0 + listed[parts * groups:]).astype(i32)
        seeds = jnp.where(mine[:, :SEEDS] > 0.0, rank[:, :SEEDS], -1)
        for o in range(groups):
            for h in range(parts):
                req_send[o, k:k + 1, h * LANES:(h + 1) * LANES] = listed[h * groups + o:h * groups + o + 1]
            req_send[o, k:k + 1, cap:] = seeds[o:o + 1]

    def order(i):
        return i + 2 if i < items - 2 else items - 1 - i

    def request_copy(t):
        to = g ^ (CORES * t + core)
        return remote(req_send.at[to], req_recv.at[t], req_ss.at[t], req_rs.at[t], to, m)

    for i in range(items):
        t = order(i)
        if t == 0:
            @pl.when(core > 0)
            def _():
                request_copy(0).start()

            @pl.when(core == 0)
            def _():
                req_recv[0] = req_send[g]
        else:
            request_copy(t).start()

    slots = lax.broadcasted_iota(i32, (1, edge_total), 1)
    banks = lax.broadcasted_iota(i32, (blocks, edge_total), 0)
    ones8 = jnp.ones((8, LANES), bf16)
    for j in range(SHARE):
        r = core * SHARE + j
        kind = RELATION_SOURCE[j] + core * (RELATION_SOURCE[SHARE + j] - RELATION_SOURCE[j])
        wanted = src[pl.ds(r, 1), :]
        found = jnp.dot(table[kind], hits(wanted & (LANES - 1), LANES), preferred_element_type=f32)
        found = found[:blocks] * 256.0 + found[blocks:]
        found = jnp.where(banks == (wanted >> log2(LANES)), found, 0.0)
        place = jnp.sum(found, axis=0, keepdims=True).astype(i32)
        live = slots < count[0, r]
        ends = dst[pl.ds(r, 1), :]
        info_send[j:j + 1, :edge_total] = jnp.where(live, place * SEEDS + ends, -1)
        marks = hits(jnp.where(live, ends, -1), SEEDS)
        tally = marks[:, :LANES]
        for base in range(LANES, edge_total, LANES):
            tally = tally + marks[:, base:base + LANES]
        tally = lax.dot_general(ones8, tally, NT, preferred_element_type=f32)
        info_send[j:j + 1, edge_total:] = tally[:1].astype(i32)

    def info_copy(d):
        return remote(info_send, info_recv.at[d // CORES, core], info_ss.at[d], info_rs.at[d // CORES, core],
                      g ^ d, plane * CORES + d % CORES)

    for i in range(items):
        for c in reversed(range(CORES)):
            d = CORES * order(i) + c
            if d == 0:
                @pl.when(core > 0)
                def _():
                    info_copy(0).start()

                @pl.when(core == 0)
                def _():
                    info_recv[0, 0] = info_send[...]
            else:
                info_copy(d).start()

    def info_wait(t, c):
        remote(info_send, info_recv.at[t, c], info_ss.at[0], info_rs.at[t, c], g, mate).wait_recv()

    def x_copy(i, w, e, t):
        to = lax.rem(plane + e, planes) * CORES + core
        return remote(xsend.at[i, t, w, e], xrecv.at[i, t, w, e], x_ss.at[i, t, w, e], x_rs.at[i, t, w, e], g, to)

    def y_copy(i, t):
        return remote(xsend.at[i, t, 1], yrecv.at[i, t], y_ss.at[i, t], y_rs.at[i, t], g ^ 1, plane * CORES)

    def z_copy(i, d, c, t, w):
        return remote(zsend.at[i, t, w, c], zrecv.at[d, t, w], z_ss.at[i, t, w, c], z_rs.at[d, t, w],
                      g ^ d, plane * CORES + c)

    def far(e, d):
        return d if e == 0 else groups + (e - 1) * CORES + d

    def own_copy(e, c, t, d):
        return remote(xsend.at[items - 1, t, :, e, c], zrecv.at[far(e, d), t], own_ss.at[t, e, c], own_rs.at[t, e, d],
                      g ^ d, lax.rem(plane + e, planes) * CORES + c)

    def spot(i):
        return jnp.where(i < items - 2, i + 2, items - 1 - i)

    def merge(i):
        for n in range(kinds):
            y_copy(i, n).wait_recv()
            for e in range(planes):
                for c in range(CORES):
                    total = xsend[i, n, 1, e, c].astype(f32) + yrecv[i, n, e, c].astype(f32)
                    xsend[i, n, 1, e, c] = total.astype(bf16)
            for e in range(1, planes):
                x_copy(i, 1, e, n).start()

    def deliver(i, w):
        d = CORES * spot(i) + core
        for n in range(kinds):
            for e in range(1, planes):
                x_copy(i, w, e, n).wait_recv()
            for c in range(CORES):
                total = xsend[i, n, w, 0, c].astype(f32)
                for e in range(1, planes):
                    total = total + xrecv[i, n, w, e, c].astype(f32)
                zsend[i, n, w, c] = total.astype(bf16)
            for c in range(CORES):
                z_copy(i, d, c, n, w).start()

    def pick(t, where):
        for k in range(kinds):
            wanted = req_recv[t, k:k + 1, :cap]
            bank = wanted >> log2(low)
            fine = wanted & (low - 1)
            choice = jnp.concatenate(
                [hits(jnp.where((fine >= base) & (fine < base + STEP), fine - base, -1), STEP)
                 for base in range(0, low, STEP)], axis=0)
            table_k = feats[k].reshape(both, rows)
            table_k = jnp.concatenate([table_k[:, h * low:(h + 1) * low] for h in range(high)], axis=0)
            found = jnp.dot(table_k, choice, preferred_element_type=f32)
            chosen = found[:both]
            for h in range(1, high):
                chosen = jnp.where(bank == h, found[h * both:(h + 1) * both], chosen)
            picked[where, k] = chosen.astype(bf16).T

    def build(place, ref_l, ref_r, n, width):
        left = hits(ref_l[pl.ds(n, 1), :width], lo_n) if width <= STEP else jnp.concatenate(
            [hits(ref_l[pl.ds(n, 1), base:base + STEP], lo_n) for base in range(0, width, STEP)], axis=1)
        right = hits(ref_r[pl.ds(n, 1), :width], hi_n * SEEDS) if width <= STEP else jnp.concatenate(
            [hits(ref_r[pl.ds(n, 1), base:base + STEP], hi_n * SEEDS) for base in range(0, width, STEP)], axis=1)
        counts = lax.dot_general(right, left, NT, preferred_element_type=f32).astype(bf16)
        for h in range(hi_n):
            adj[place, :, h * lo_n:(h + 1) * lo_n] = counts[h * SEEDS:(h + 1) * SEEDS]

    def item(i, first, last):
        t = order(i) if first or last else spot(i)
        where = 1 if last else 0
        if not last:
            request_copy(t).wait_recv()
            pick(t, 0)
        if last:
            @pl.when(core > 0)
            def _():
                info_wait(t, 0)
        else:
            info_wait(t, 0)
        info_wait(t, 1)
        if first:
            loads[kinds].wait()
            swaps[kinds].wait()
        for c in range(CORES):
            packed = info_recv[t, c, :, :edge_total] - g * (cap * SEEDS)
            ok = (packed >= 0) & (packed < cap * SEEDS)
            slot = packed >> log2(SEEDS)
            lidx[c * SHARE:(c + 1) * SHARE, :] = (slot & (lo_n - 1)).astype(f32)
            ridx[c * SHARE:(c + 1) * SHARE, :] = jnp.where(
                ok, (slot >> log2(lo_n)) * SEEDS + (packed & (SEEDS - 1)), -1).astype(f32)
        slot = req_recv[t, :, cap:]
        lidx[RELS:RELS + kinds, :SEEDS] = (slot & (lo_n - 1)).astype(f32)
        ridx[RELS:RELS + kinds, :SEEDS] = jnp.where(
            slot >= 0, (slot >> log2(lo_n)) * SEEDS + lax.broadcasted_iota(i32, slot.shape, 1), -1).astype(f32)
        degree = jnp.concatenate([info_recv[t, c, :, edge_total:] for c in range(CORES)], axis=0)
        inverse = (1.0 / jnp.maximum(degree.astype(f32), 1.0)).T
        groups_of = [[matrix for matrix in range(MATS) if MATRIX_TARGET[matrix] == n] for n in range(kinds)]

        def make(matrix):
            build(matrix, lidx, ridx, matrix, edge_total if matrix < RELS else SEEDS)

        def gather(n):
            values = []
            for matrix in groups_of[n]:
                kind = RELATION_SOURCE[matrix] if matrix < RELS else matrix - RELS
                value = jnp.dot(adj[matrix], picked[where, kind], preferred_element_type=f32)
                if matrix < RELS:
                    value = value * inverse[:, matrix:matrix + 1]
                values.append(value.astype(bf16))
            return jnp.concatenate(values, axis=1)

        def emit(n, left):
            right = jnp.concatenate([weights[c, matrix] for matrix in groups_of[n] for c in range(CORES)], axis=0)
            typed = jnp.dot(left, right, preferred_element_type=f32).astype(bf16)
            for p in range(planes):
                for w in range(WAYS):
                    for c in range(CORES):
                        xsend[i, n, w, lax.rem(p - plane + planes, planes), c] = typed[
                            w * span:(w + 1) * span, p * half + c * quarter:p * half + (c + 1) * quarter]
            if last:
                for e in reversed(range(planes)):
                    for c in range(CORES):
                        if e or c:
                            own_copy(e, c, n, core).start()

                @pl.when(core > 0)
                def _():
                    own_copy(0, 0, n, core).start()

                @pl.when(core == 0)
                def _():
                    for w in range(WAYS):
                        zrecv[0, n, w] = xsend[i, n, w, 0, 0]
            else:
                for e in range(1, planes):
                    x_copy(i, 0, e, n).start()

                @pl.when(core > 0)
                def _():
                    y_copy(i, n).start()

        for matrix in groups_of[0] + groups_of[1][:1]:
            make(matrix)
        left = gather(0)
        make(groups_of[1][1])
        emit(0, left)
        if not first:
            @pl.when((i >= 2) & (core == 0))
            def _():
                deliver(i - 2, 1)

            @pl.when(core == 0)
            def _():
                merge(i - 1)

            deliver(i - 1, 0)
        for matrix in groups_of[1][2:] + groups_of[2][:1]:
            make(matrix)
        left = gather(1)
        for matrix in groups_of[2][1:]:
            make(matrix)
        emit(1, left)
        emit(2, gather(2))
        if last:
            @pl.when(core == 0)
            def _():
                deliver(i - 1, 1)

    def rest(i, _):
        item(i, False, False)
        return 0

    for k in range(kinds):
        loads[k].wait()
        swaps[k].wait()

    @pl.when(core > 0)
    def _():
        request_copy(0).wait_recv()
    pick(0, 1)
    item(0, True, False)
    lax.fori_loop(1, items - 1, rest, 0)
    item(items - 1, False, True)

    for n in range(kinds):
        halves = []
        for w in range(WAYS):
            total = jnp.zeros((span, quarter), f32)
            for i in range(items - 1):
                for c in range(CORES if w == 0 else 1):
                    d = CORES * order(i) + c
                    z_copy(0, d, 0, n, w).wait_recv()
                    total = total + zrecv[d, n, w].astype(f32)
            halves.append(total)
        for e in range(planes):
            for d in range(CORES):
                if e or d:
                    own_copy(e, 0, n, d).wait_recv()
                else:
                    @pl.when(core > 0)
                    def _():
                        own_copy(0, 0, n, 0).wait_recv()
                for w in range(WAYS):
                    halves[w] = halves[w] + zrecv[far(e, d), n, w].astype(f32)
        total = jnp.concatenate(halves, axis=0)
        out[n] = jnp.maximum(total, 0.0).T.astype(bf16)

    for t in range(items):
        if t == 0:
            @pl.when(core > 0)
            def _():
                request_copy(0).wait_send()
                info_copy(0).wait_send()
        else:
            request_copy(t).wait_send()
            info_copy(CORES * t).wait_send()
        for c in range(1, CORES):
            info_copy(CORES * t + c).wait_send()
    for i in range(items - 1):
        d = CORES * order(i) + core
        for n in range(kinds):
            for e in range(1, planes):
                x_copy(i, 0, e, n).wait_send()
            for c in range(CORES):
                z_copy(i, d, c, n, 0).wait_send()

        @pl.when(core == 0)
        def _():
            for n in range(kinds):
                for e in range(1, planes):
                    x_copy(i, 1, e, n).wait_send()
                for c in range(CORES):
                    z_copy(i, d, c, n, 1).wait_send()

        @pl.when(core > 0)
        def _():
            for n in range(kinds):
                y_copy(i, n).wait_send()
    for n in range(kinds):
        for e in range(planes):
            for c in range(CORES):
                if e or c:
                    own_copy(e, c, n, core).wait_send()

        @pl.when(core > 0)
        def _():
            own_copy(0, 0, n, core).wait_send()


def per_device(features, weights, sample_owner, sample_row, edge_src, edge_dst, edge_count):
    groups, shares = lax.axis_size("dp"), lax.axis_size("mp")
    kinds, feat, rows = features.shape
    sampled, edge_total = sample_row.shape[1], edge_src.shape[1]
    cap = 2 * sampled // groups
    items, planes = groups // CORES, shares // CORES
    width = weights.shape[2]
    quarter = width // shares
    bf16, f32, i32 = jnp.bfloat16, jnp.float32, jnp.int32
    vmem = pl.BlockSpec(memory_space=pltpu.VMEM)
    any_space = pl.BlockSpec(memory_space=pl.ANY)
    dma = pltpu.SemaphoreType.DMA
    return pl.pallas_call(
        functools.partial(kernel, groups, shares),
        out_shape=jax.ShapeDtypeStruct((kinds, quarter, SEEDS), bf16),
        in_specs=[any_space] * 2 + [vmem] * 4 + [pl.BlockSpec(memory_space=pltpu.SMEM)],
        out_specs=vmem,
        scratch_shapes=[
            pltpu.VMEM((kinds, CORES, feat, rows), bf16),
            pltpu.VMEM((CORES, MATS, feat, width), bf16),
            pltpu.VMEM((STEP, max(sampled, edge_total)), bf16),
            pltpu.VMEM((groups, kinds, cap + SEEDS), i32),
            pltpu.VMEM((items, kinds, cap + SEEDS), i32),
            pltpu.VMEM((SHARE, edge_total + SEEDS), i32),
            pltpu.VMEM((items, CORES, SHARE, edge_total + SEEDS), i32),
            pltpu.VMEM((kinds, 2 * sampled // LANES, LANES), bf16),
            pltpu.VMEM((16, edge_total), f32),
            pltpu.VMEM((16, edge_total), f32),
            pltpu.VMEM((2, kinds, cap, CORES * feat), bf16),
            pltpu.VMEM((MATS, SEEDS, cap), bf16),
            pltpu.VMEM((items, kinds, WAYS, planes, CORES, SEEDS // WAYS, quarter), bf16),
            pltpu.VMEM((items, kinds, WAYS, planes, CORES, SEEDS // WAYS, quarter), bf16),
            pltpu.VMEM((items, kinds, planes, CORES, SEEDS // WAYS, quarter), bf16),
            pltpu.VMEM((items, kinds, WAYS, CORES, SEEDS // WAYS, quarter), bf16),
            pltpu.VMEM((groups + (planes - 1) * CORES, kinds, WAYS, SEEDS // WAYS, quarter), bf16),
            dma((kinds + 1,)), dma((kinds + 1,)), dma((kinds + 1,)),
            dma((items,)), dma((items,)),
            dma((groups,)), dma((items, CORES)),
            dma((items, kinds, WAYS, planes)), dma((items, kinds, WAYS, planes)),
            dma((items, kinds)), dma((items, kinds)),
            dma((items, kinds, WAYS, CORES)), dma((groups, kinds, WAYS)),
            dma((kinds, planes, CORES)), dma((kinds, planes, CORES)),
        ],
        compiler_params=pltpu.CompilerParams(
            collective_id=0, has_side_effects=True, vmem_limit_bytes=60 * 1024 * 1024),
    )(features, weights, sample_owner.transpose(0, 2, 1), sample_row, edge_src, edge_dst, edge_count.T)


def solution(mesh):
    return jax.shard_map(
        per_device,
        mesh=mesh,
        in_specs=(
            P(None, "mp", "dp"),
            P(None, "mp", None),
            P(None, "dp", None),
            P(None, "dp"),
            P(None, "dp"),
            P(None, "dp"),
            P(None, "dp"),
        ),
        out_specs=P(None, "mp", "dp"),
        check_vma=False,
    )
```

```python
import functools

import jax
import jax.numpy as jnp
from jax import lax
from jax.experimental import pallas as pl
from jax.experimental.pallas import tpu as pltpu
from jax.sharding import PartitionSpec as P

SEEDS = 128
RELATION_SOURCE = (0, 1, 0, 1, 2, 0, 2, 1)
MATRIX_TARGET = (1, 0, 0, 2, 1, 2, 0, 1, 0, 1, 2)
RELS = len(RELATION_SOURCE)
KINDS = 3
MATS = RELS + KINDS
SLOTS = tuple(
    tuple([r for r in range(RELS) if RELATION_SOURCE[r] == k] + [RELS + k]) for k in range(KINDS)
)
ORDER = tuple(m for group in SLOTS for m in group)
STARTS = tuple(sum(len(group) for group in SLOTS[:k]) for k in range(KINDS))
PLACE = tuple(ORDER.index(m) for m in range(MATS))
CORES = 2
WAYS = 2
SHARE = RELS // CORES
STEP = 256
LANES = 128
ONE_HOT = jnp.float8_e4m3fn
MESH = pl.DeviceIdType.MESH
NT = (((1,), (1,)), ((), ()))


def log2(n):
    return n.bit_length() - 1


def kernel(groups, shares, features_in, weights_in, owner_in, row_in, src_in, dst_in, count, out,
           owner, row, src, dst, feats, weights, req_send, req_recv, info_send, info_recv, table,
           lidx, ridx, picked, adj, xsend, xrecv, yrecv, zsend, zrecv,
           in_sem, list_sem, fx_ss, fx_rs, req_ss, req_rs, info_ss, info_rs, x_ss, x_rs, y_ss, y_rs, z_ss, z_rs, own_ss, own_rs, near_ss, near_rs):
    kinds, _, feat, rows = feats.shape
    both = CORES * feat
    sampled = row.shape[1]
    edge_total = src.shape[1]
    cap = req_send.shape[2] - SEEDS
    low = min(512, rows)
    high = rows // low
    lo_n = min(STEP, cap)
    hi_n = cap // lo_n
    items = groups // CORES
    planes = shares // CORES
    quarter = xsend.shape[6]
    span = SEEDS // WAYS
    half = CORES * quarter
    g = lax.axis_index("dp")
    m = lax.axis_index("mp")
    core = lax.rem(m, CORES)
    plane = m // CORES
    f32, bf16, i32 = jnp.float32, jnp.bfloat16, jnp.int32

    def at(group, mp):
        return {"dp": group, "mp": mp}

    def remote(source, target, ss, rs, group, mp):
        return pltpu.make_async_remote_copy(source, target, ss, rs, device_id=at(group, mp), device_id_type=MESH)

    def levels(size):
        return lax.broadcasted_iota(i32, (size, LANES), 0).astype(f32).astype(bf16)

    def hits(index, size, kind=bf16):
        level = levels(size)
        index = index.astype(f32).astype(bf16)
        yes, no = jnp.ones((), kind), jnp.zeros((), kind)
        return jnp.concatenate(
            [jnp.where(level == index[:, base:base + LANES], yes, no)
             for base in range(0, index.shape[1], LANES)], axis=1)

    mate = m - core + lax.rem(core + 1, CORES)
    loads, swaps = [], []
    for k in range(kinds):
        loads.append(pltpu.make_async_copy(features_in.at[k], feats.at[k, 0], in_sem.at[k]))
        swaps.append(remote(features_in.at[k], feats.at[k, 1], fx_ss.at[k], fx_rs.at[k], g, mate))
    loads.append(pltpu.make_async_copy(weights_in, weights.at[0], in_sem.at[kinds]))
    swaps.append(remote(weights_in, weights.at[1], fx_ss.at[kinds], fx_rs.at[kinds], g, mate))
    lists = [pltpu.make_async_copy(source, target, list_sem.at[n]) for n, (source, target) in enumerate(
        ((owner_in, owner), (row_in, row), (src_in, src), (dst_in, dst)))]
    for copy in lists + loads:
        copy.start()

    barrier = pltpu.get_barrier_semaphore()
    pl.semaphore_signal(barrier, inc=1, device_id=at(g, mate), device_id_type=MESH)
    for d in range(1, groups):
        for c in range(CORES):
            pl.semaphore_signal(barrier, inc=1, device_id=at(g ^ d, plane * CORES + c), device_id_type=MESH)
    for e in range(1, planes):
        pl.semaphore_signal(
            barrier, inc=1, device_id=at(g, lax.rem(plane + e, planes) * CORES + core), device_id_type=MESH)
    pl.semaphore_wait(barrier, CORES * (groups - 1) + planes)
    for copy in swaps:
        copy.start()
    for copy in lists:
        copy.wait()

    tri = (lax.broadcasted_iota(i32, (STEP, STEP), 0) <= lax.broadcasted_iota(i32, (STEP, STEP), 1))
    tri = jnp.where(tri, 1.0, 0.0).astype(bf16)
    hot = jnp.concatenate([
        jnp.where(lax.broadcasted_iota(i32, (groups, sampled), 0) == owner[k], 1.0, 0.0)
        for k in range(kinds)], axis=0)
    lines = kinds * groups
    pieces = [hot[:, base:base + STEP] for base in range(0, sampled, STEP)]
    upto = jnp.dot(jnp.concatenate(pieces, axis=0).astype(bf16), tri, preferred_element_type=f32)
    carry = jnp.zeros((lines, 1), f32)
    ranks = []
    for n, piece in enumerate(pieces):
        here = upto[n * lines:(n + 1) * lines]
        ranks.append((here + (carry - 1.0)) * piece)
        carry = carry + here[:, STEP - 1:]
    ranks = jnp.concatenate(ranks, axis=1)

    blocks = sampled // LANES
    parts = cap // LANES
    for k in range(kinds):
        mine = hot[k * groups:(k + 1) * groups]
        rank = jnp.sum(ranks[k * groups:(k + 1) * groups], axis=0, keepdims=True).astype(i32)
        place = owner[k] * cap + rank
        coarse = (place >> 8).astype(f32)
        fine = (place & 255).astype(f32)
        table[k] = jnp.concatenate(
            [part[:, b * LANES:(b + 1) * LANES] for part in (coarse, fine) for b in range(blocks)], axis=0).astype(bf16)
        wanted = row[k:k + 1, :]
        tall = mine * (wanted >> 8).astype(f32)
        wide = mine * (wanted & 255).astype(f32)
        bank = rank >> log2(LANES)
        stack = jnp.concatenate(
            [jnp.where(bank == h, part, 0.0) for part in (tall, wide) for h in range(parts)], axis=0).astype(bf16)
        listed = lax.dot_general(stack, hits(rank & (LANES - 1), LANES), NT, preferred_element_type=f32)
        listed = (listed[:parts * groups] * 256.0 + listed[parts * groups:]).astype(i32)
        seeds = jnp.where(mine[:, :SEEDS] > 0.0, rank[:, :SEEDS], -1)
        for o in range(groups):
            for h in range(parts):
                req_send[o, k:k + 1, h * LANES:(h + 1) * LANES] = listed[h * groups + o:h * groups + o + 1]
            req_send[o, k:k + 1, cap:] = seeds[o:o + 1]

    def order(i):
        return i + 2 if i < items - 2 else items - 1 - i

    def request_copy(t):
        to = g ^ (CORES * t + core)
        return remote(req_send.at[to], req_recv.at[t], req_ss.at[t], req_rs.at[t], to, m)

    for i in range(items):
        t = order(i)
        if t == 0:
            @pl.when(core > 0)
            def _():
                request_copy(0).start()

            @pl.when(core == 0)
            def _():
                req_recv[0] = req_send[g]
        else:
            request_copy(t).start()

    slots = lax.broadcasted_iota(i32, (1, edge_total), 1)
    banks = lax.broadcasted_iota(i32, (blocks, edge_total), 0)
    ones8 = jnp.ones((8, LANES), bf16)
    for j in range(SHARE):
        r = core * SHARE + j
        kind = RELATION_SOURCE[j] + core * (RELATION_SOURCE[SHARE + j] - RELATION_SOURCE[j])
        wanted = src[pl.ds(r, 1), :]
        found = jnp.dot(table[kind], hits(wanted & (LANES - 1), LANES), preferred_element_type=f32)
        found = found[:blocks] * 256.0 + found[blocks:]
        found = jnp.where(banks == (wanted >> log2(LANES)), found, 0.0)
        place = jnp.sum(found, axis=0, keepdims=True).astype(i32)
        live = slots < count[0, r]
        ends = dst[pl.ds(r, 1), :]
        info_send[j:j + 1, :edge_total] = jnp.where(live, place * SEEDS + ends, -1)
        marks = hits(jnp.where(live, ends, -1), SEEDS)
        tally = marks[:, :LANES]
        for base in range(LANES, edge_total, LANES):
            tally = tally + marks[:, base:base + LANES]
        tally = lax.dot_general(ones8, tally, NT, preferred_element_type=f32)
        info_send[j:j + 1, edge_total:] = tally[:1].astype(i32)

    def info_copy(d):
        return remote(info_send, info_recv.at[d // CORES, core], info_ss.at[d], info_rs.at[d // CORES, core],
                      g ^ d, plane * CORES + d % CORES)

    for i in range(items):
        for c in reversed(range(CORES)):
            d = CORES * order(i) + c
            if d == 0:
                @pl.when(core > 0)
                def _():
                    info_copy(0).start()

                @pl.when(core == 0)
                def _():
                    info_recv[0, 0] = info_send[...]
            else:
                info_copy(d).start()

    def info_wait(t, c):
        remote(info_send, info_recv.at[t, c], info_ss.at[0], info_rs.at[t, c], g, mate).wait_recv()

    def x_copy(i, w, e, t=slice(None)):
        to = lax.rem(plane + e, planes) * CORES + core
        return remote(xsend.at[i, t, w, e], xrecv.at[i, t, w, e], x_ss.at[i, w, e], x_rs.at[i, w, e], g, to)

    def y_copy(i, t=slice(None)):
        return remote(xsend.at[i, t, 1], yrecv.at[i, t], y_ss.at[i], y_rs.at[i], g ^ 1, plane * CORES)

    def z_copy(i, d, w, c, t):
        return remote(zsend.at[i, t, w, c], zrecv.at[d, t, w], z_ss.at[i, w], z_rs.at[d, w],
                      g ^ d, plane * CORES + c)

    near = items - 2

    def side(e):
        return CORES * order(near) if e == 0 else groups + (planes - 1) * CORES + e - 1

    def near_copy(e, c):
        return remote(xsend.at[near, :, 1, e, c], zrecv.at[side(e), :, 1], near_ss.at[e, c], near_rs.at[e],
                      g ^ (CORES * order(near)), lax.rem(plane + e, planes) * CORES + c)

    def z_sent(i, w):
        return remote(zsend.at[i, :, w], zsend.at[i, :, w], z_ss.at[i, w], z_rs.at[0, w], g, mate)

    def z_landed(d, w):
        return remote(zrecv.at[d, :, w], zrecv.at[d, :, w], z_ss.at[0, w], z_rs.at[d, w], g, mate)

    def far(e, d):
        return d if e == 0 else groups + (e - 1) * CORES + d

    def own_copy(e, c, d, t=slice(None)):
        return remote(xsend.at[items - 1, t, :, e, c], zrecv.at[far(e, d), t], own_ss.at[e, c], own_rs.at[e, d],
                      g ^ d, lax.rem(plane + e, planes) * CORES + c)

    def spot(i):
        return jnp.where(i < items - 2, i + 2, items - 1 - i)

    def merge(i):
        y_copy(i).wait_recv()
        for n in range(kinds):
            for e in range(planes):
                for c in range(CORES):
                    total = xsend[i, n, 1, e, c].astype(f32) + yrecv[i, n, e, c].astype(f32)
                    xsend[i, n, 1, e, c] = total.astype(bf16)
        for e in reversed(range(planes)):
            if isinstance(i, int) and i == near:
                for c in range(CORES):
                    near_copy(e, c).start()
            elif e:
                x_copy(i, 1, e).start()

    def deliver(i, w):
        d = CORES * spot(i) + core
        for e in range(1, planes):
            x_copy(i, w, e).wait_recv()
        for n in range(kinds):
            for c in range(CORES):
                total = xsend[i, n, w, 0, c].astype(f32)
                for e in range(1, planes):
                    total = total + xrecv[i, n, w, e, c].astype(f32)
                zsend[i, n, w, c] = total.astype(bf16)
        for c in range(CORES):
            z_copy(i, d, w, c, slice(None)).start()

    def pick(t, where, sides):
        tall = len(sides) * feat
        for k in range(kinds):
            wanted = req_recv[t, k:k + 1, :cap]
            bank = wanted >> log2(low)
            fine = wanted & (low - 1)
            choice = jnp.concatenate(
                [hits(jnp.where((fine >= base) & (fine < base + STEP), fine - base, -1), STEP)
                 for base in range(0, low, STEP)], axis=0)
            rows_k = jnp.concatenate(
                [feats[k, c, :, h * low:(h + 1) * low] for h in range(high) for c in sides], axis=0)
            found = jnp.dot(rows_k, choice, preferred_element_type=f32)
            chosen = found[:tall]
            for h in range(1, high):
                chosen = jnp.where(bank == h, found[h * tall:(h + 1) * tall], chosen)
            picked[where, k, :, sides[0] * feat:(sides[-1] + 1) * feat] = chosen.astype(bf16).T

    def build(place, ref_l, ref_r, n, width):
        left = hits(ref_l[n:n + 1, :width], lo_n, ONE_HOT)
        right = hits(ref_r[n:n + 1, :width], hi_n * SEEDS, ONE_HOT)
        counts = lax.dot_general(right, left, NT, preferred_element_type=f32).astype(bf16)
        for h in range(hi_n):
            adj[place, :, h * lo_n:(h + 1) * lo_n] = counts[h * SEEDS:(h + 1) * SEEDS]

    def item(i, first, last):
        t = order(i) if first or last else spot(i)
        where = 1 if last else 0
        if not last:
            request_copy(t).wait_recv()
            pick(t, 0, range(CORES))
        if last:
            @pl.when(core > 0)
            def _():
                info_wait(t, 0)
        else:
            info_wait(t, 0)
        info_wait(t, 1)
        if first:
            loads[kinds].wait()
            swaps[kinds].wait()
        for c in range(CORES):
            packed = info_recv[t, c, :, :edge_total] - g * (cap * SEEDS)
            ok = (packed >= 0) & (packed < cap * SEEDS)
            slot = packed >> log2(SEEDS)
            lidx[c * SHARE:(c + 1) * SHARE, :] = (slot & (lo_n - 1)).astype(f32)
            ridx[c * SHARE:(c + 1) * SHARE, :] = jnp.where(
                ok, (slot >> log2(lo_n)) * SEEDS + (packed & (SEEDS - 1)), -1).astype(f32)
        slot = req_recv[t, :, cap:]
        lidx[RELS:RELS + kinds, :SEEDS] = (slot & (lo_n - 1)).astype(f32)
        ridx[RELS:RELS + kinds, :SEEDS] = jnp.where(
            slot >= 0, (slot >> log2(lo_n)) * SEEDS + lax.broadcasted_iota(i32, slot.shape, 1), -1).astype(f32)
        degree = jnp.concatenate([info_recv[t, c, :, edge_total:] for c in range(CORES)], axis=0)
        inverse = (1.0 / jnp.maximum(degree.astype(f32), 1.0)).T
        groups_of = [[matrix for matrix in range(MATS) if MATRIX_TARGET[matrix] == n] for n in range(kinds)]

        def make(matrix):
            build(matrix, lidx, ridx, matrix, edge_total if matrix < RELS else SEEDS)

        def gather(n):
            values = []
            for matrix in groups_of[n]:
                kind = RELATION_SOURCE[matrix] if matrix < RELS else matrix - RELS
                value = jnp.dot(adj[matrix], picked[where, kind], preferred_element_type=f32)
                if matrix < RELS:
                    value = value * inverse[:, matrix:matrix + 1]
                values.append(value.astype(bf16))
            return jnp.concatenate(values, axis=1)

        def emit(n, left):
            right = jnp.concatenate([weights[c, matrix] for matrix in groups_of[n] for c in range(CORES)], axis=0)
            typed = jnp.dot(left, right, preferred_element_type=f32).astype(bf16)
            for p in range(planes):
                for w in range(WAYS):
                    for c in range(CORES):
                        xsend[i, n, w, lax.rem(p - plane + planes, planes), c] = typed[
                            w * span:(w + 1) * span, p * half + c * quarter:p * half + (c + 1) * quarter]
            if last:
                for e in reversed(range(planes)):
                    for c in range(CORES):
                        if e or c:
                            own_copy(e, c, core, n).start()

                @pl.when(core > 0)
                def _():
                    own_copy(0, 0, core, n).start()

                @pl.when(core == 0)
                def _():
                    for w in range(WAYS):
                        zrecv[0, n, w] = xsend[i, n, w, 0, 0]
            else:
                for e in range(1, planes):
                    x_copy(i, 0, e, n).start()

                @pl.when(core > 0)
                def _():
                    y_copy(i, n).start()

        for matrix in groups_of[0] + groups_of[1][:1]:
            make(matrix)
        left = gather(0)
        make(groups_of[1][1])
        emit(0, left)
        def relay():
            @pl.when((i >= 2) & (core == 0))
            def _():
                deliver(i - 2, 1)

        def advance():
            @pl.when(core == 0)
            def _():
                merge(i - 1)

            deliver(i - 1, 0)

        if not first:
            relay()
        if not first and not last:
            advance()
        for matrix in groups_of[1][2:] + groups_of[2][:1]:
            make(matrix)
        left = gather(1)
        for matrix in groups_of[2][1:]:
            make(matrix)
        emit(1, left)
        if last:
            advance()
        emit(2, gather(2))

    def rest(i, _):
        item(i, False, False)
        return 0

    for k in range(kinds):
        loads[k].wait()

    @pl.when(core > 0)
    def _():
        request_copy(0).wait_recv()
    pick(0, 1, (0,))
    for k in range(kinds):
        swaps[k].wait()
    pick(0, 1, (1,))
    item(0, True, False)
    lax.fori_loop(1, items - 1, rest, 0)
    item(items - 1, False, True)

    pieces = []
    for i in range(items - 1):
        for w in range(WAYS):
            for c in range(CORES if w == 0 else 1):
                d = CORES * order(i) + c
                if w == 0 or i < near:
                    z_landed(d, w).wait_recv()
                    pieces.append((w, d))
    for e in range(planes):
        near_copy(e, 0).wait_recv()
        pieces.append((1, side(e)))
    for e in range(planes):
        for d in range(CORES):
            if e or d:
                own_copy(e, 0, d).wait_recv()
            else:
                @pl.when(core > 0)
                def _():
                    own_copy(0, 0, 0).wait_recv()
            for w in range(WAYS):
                pieces.append((w, far(e, d)))
    for n in range(kinds):
        halves = []
        for w in range(WAYS):
            total = jnp.zeros((span, quarter), f32)
            for v, place in pieces:
                if v == w:
                    total = total + zrecv[place, n, w].astype(f32)
            halves.append(total)
        out[n] = jnp.maximum(jnp.concatenate(halves, axis=0), 0.0).T.astype(bf16)
    for t in range(items):
        if t == 0:
            @pl.when(core > 0)
            def _():
                request_copy(0).wait_send()
                info_copy(0).wait_send()
        else:
            request_copy(t).wait_send()
            info_copy(CORES * t).wait_send()
        for c in range(1, CORES):
            info_copy(CORES * t + c).wait_send()
    for i in range(items - 1):
        for e in range(1, planes):
            x_copy(i, 0, e).wait_send()
        z_sent(i, 0).wait_send()

        @pl.when(core == 0)
        def _():
            if i < near:
                for e in range(1, planes):
                    x_copy(i, 1, e).wait_send()
                z_sent(i, 1).wait_send()
            else:
                for e in range(planes):
                    for c in range(CORES):
                        near_copy(e, c).wait_send()

        @pl.when(core > 0)
        def _():
            y_copy(i).wait_send()
    for e in range(planes):
        for c in range(CORES):
            if e or c:
                own_copy(e, c, core).wait_send()

    @pl.when(core > 0)
    def _():
        own_copy(0, 0, core).wait_send()


def per_device(features, weights, sample_owner, sample_row, edge_src, edge_dst, edge_count):
    groups, shares = lax.axis_size("dp"), lax.axis_size("mp")
    kinds, feat, rows = features.shape
    sampled, edge_total = sample_row.shape[1], edge_src.shape[1]
    cap = 2 * sampled // groups
    items, planes = groups // CORES, shares // CORES
    width = weights.shape[2]
    quarter = width // shares
    bf16, f32, i32 = jnp.bfloat16, jnp.float32, jnp.int32
    vmem = pl.BlockSpec(memory_space=pltpu.VMEM)
    any_space = pl.BlockSpec(memory_space=pl.ANY)
    dma = pltpu.SemaphoreType.DMA
    return pl.pallas_call(
        functools.partial(kernel, groups, shares),
        out_shape=jax.ShapeDtypeStruct((kinds, quarter, SEEDS), bf16),
        in_specs=[any_space] * 6 + [pl.BlockSpec(memory_space=pltpu.SMEM)],
        out_specs=vmem,
        scratch_shapes=[
            pltpu.VMEM((kinds, 1, sampled), i32),
            pltpu.VMEM((kinds, sampled), i32),
            pltpu.VMEM(edge_src.shape, i32),
            pltpu.VMEM(edge_src.shape, i32),
            pltpu.VMEM((kinds, CORES, feat, rows), bf16),
            pltpu.VMEM((CORES, MATS, feat, width), bf16),
            pltpu.VMEM((groups, kinds, cap + SEEDS), i32),
            pltpu.VMEM((items, kinds, cap + SEEDS), i32),
            pltpu.VMEM((SHARE, edge_total + SEEDS), i32),
            pltpu.VMEM((items, CORES, SHARE, edge_total + SEEDS), i32),
            pltpu.VMEM((kinds, 2 * sampled // LANES, LANES), bf16),
            pltpu.VMEM((16, edge_total), f32),
            pltpu.VMEM((16, edge_total), f32),
            pltpu.VMEM((2, kinds, cap, CORES * feat), bf16),
            pltpu.VMEM((MATS, SEEDS, cap), bf16),
            pltpu.VMEM((items, kinds, WAYS, planes, CORES, SEEDS // WAYS, quarter), bf16),
            pltpu.VMEM((items, kinds, WAYS, planes, CORES, SEEDS // WAYS, quarter), bf16),
            pltpu.VMEM((items, kinds, planes, CORES, SEEDS // WAYS, quarter), bf16),
            pltpu.VMEM((items, kinds, WAYS, CORES, SEEDS // WAYS, quarter), bf16),
            pltpu.VMEM((groups + (planes - 1) * (CORES + 1), kinds, WAYS, SEEDS // WAYS, quarter), bf16),
            dma((kinds + 1,)), dma((4,)), dma((kinds + 1,)), dma((kinds + 1,)),
            dma((items,)), dma((items,)),
            dma((groups,)), dma((items, CORES)),
            dma((items - 1, WAYS, planes)), dma((items - 1, WAYS, planes)),
            dma((items - 1,)), dma((items - 1,)),
            dma((items - 1, WAYS)), dma((groups, WAYS)),
            dma((planes, CORES)), dma((planes, CORES)),
            dma((planes, CORES)), dma((planes,)),
        ],
        compiler_params=pltpu.CompilerParams(
            collective_id=0, has_side_effects=True, vmem_limit_bytes=60 * 1024 * 1024),
    )(features, weights, sample_owner.transpose(0, 2, 1), sample_row, edge_src, edge_dst, edge_count.T)


def solution(mesh):
    return jax.shard_map(
        per_device,
        mesh=mesh,
        in_specs=(
            P(None, "mp", "dp"),
            P(None, "mp", None),
            P(None, "dp", None),
            P(None, "dp"),
            P(None, "dp"),
            P(None, "dp"),
            P(None, "dp"),
        ),
        out_specs=P(None, "mp", "dp"),
        check_vma=False,
    )
```

```python
import functools

import jax
import jax.numpy as jnp
from jax import lax
from jax.experimental import pallas as pl
from jax.experimental.pallas import tpu as pltpu
from jax.sharding import PartitionSpec as P

SEEDS = 128
RELATION_SOURCE = (0, 1, 0, 1, 2, 0, 2, 1)
MATRIX_TARGET = (1, 0, 0, 2, 1, 2, 0, 1, 0, 1, 2)
RELS = len(RELATION_SOURCE)
KINDS = 3
MATS = RELS + KINDS
SLOTS = tuple(
    tuple([r for r in range(RELS) if RELATION_SOURCE[r] == k] + [RELS + k]) for k in range(KINDS)
)
ORDER = tuple(m for group in SLOTS for m in group)
STARTS = tuple(sum(len(group) for group in SLOTS[:k]) for k in range(KINDS))
PLACE = tuple(ORDER.index(m) for m in range(MATS))
CORES = 2
WAYS = 2
SHARE = RELS // CORES
STEP = 256
LANES = 128
ONE_HOT = jnp.float8_e4m3fn
MESH = pl.DeviceIdType.MESH
NT = (((1,), (1,)), ((), ()))


def log2(n):
    return n.bit_length() - 1


def kernel(groups, shares, features_in, weights_in, owner_in, row_in, src_in, dst_in, count_in, out,
           owner, row, src, dst, count, feats, weights, req_send, req_recv, info_send, info_recv, table,
           lidx, ridx, picked, adj, xsend, xrecv, yrecv, zsend, zrecv,
           in_sem, list_sem, fx_ss, fx_rs, req_ss, req_rs, info_ss, info_rs, x_ss, x_rs, y_ss, y_rs, z_ss, z_rs, own_ss, own_rs, near_ss, near_rs):
    kinds, _, feat, rows = feats.shape
    both = CORES * feat
    sampled = row.shape[1]
    edge_total = src.shape[1]
    cap = req_send.shape[2] - SEEDS
    low = min(512, rows)
    high = rows // low
    lo_n = min(STEP, cap)
    hi_n = cap // lo_n
    items = groups // CORES
    planes = shares // CORES
    quarter = xsend.shape[6]
    span = SEEDS // WAYS
    half = CORES * quarter
    g = lax.axis_index("dp")
    m = lax.axis_index("mp")
    core = lax.rem(m, CORES)
    plane = m // CORES
    f32, bf16, i32 = jnp.float32, jnp.bfloat16, jnp.int32

    def at(group, mp):
        return {"dp": group, "mp": mp}

    def remote(source, target, ss, rs, group, mp):
        return pltpu.make_async_remote_copy(source, target, ss, rs, device_id=at(group, mp), device_id_type=MESH)

    def levels(size):
        return lax.broadcasted_iota(i32, (size, LANES), 0).astype(f32).astype(bf16)

    def hits(index, size, kind=bf16):
        level = levels(size)
        index = index.astype(f32).astype(bf16)
        yes, no = jnp.ones((), kind), jnp.zeros((), kind)
        return jnp.concatenate(
            [jnp.where(level == index[:, base:base + LANES], yes, no)
             for base in range(0, index.shape[1], LANES)], axis=1)

    mate = m - core + lax.rem(core + 1, CORES)
    loads, swaps = [], []
    for k in range(kinds):
        loads.append(pltpu.make_async_copy(features_in.at[k], feats.at[k, 0], in_sem.at[k]))
        swaps.append(remote(features_in.at[k], feats.at[k, 1], fx_ss.at[k], fx_rs.at[k], g, mate))
    loads.append(pltpu.make_async_copy(weights_in, weights.at[0], in_sem.at[kinds]))
    swaps.append(remote(weights_in, weights.at[1], fx_ss.at[kinds], fx_rs.at[kinds], g, mate))
    lists = [pltpu.make_async_copy(source, target, list_sem.at[n]) for n, (source, target) in enumerate(
        ((owner_in, owner), (row_in, row), (src_in, src), (dst_in, dst), (count_in, count)))]
    for copy in lists + loads:
        copy.start()

    barrier = pltpu.get_barrier_semaphore()
    pl.semaphore_signal(barrier, inc=1, device_id=at(g, mate), device_id_type=MESH)
    for d in range(1, groups):
        for c in range(CORES):
            pl.semaphore_signal(barrier, inc=1, device_id=at(g ^ d, plane * CORES + c), device_id_type=MESH)
    for e in range(1, planes):
        pl.semaphore_signal(
            barrier, inc=1, device_id=at(g, lax.rem(plane + e, planes) * CORES + core), device_id_type=MESH)
    pl.semaphore_wait(barrier, CORES * (groups - 1) + planes)
    for copy in swaps:
        copy.start()
    for copy in lists:
        copy.wait()

    tri = (lax.broadcasted_iota(i32, (STEP, STEP), 0) <= lax.broadcasted_iota(i32, (STEP, STEP), 1))
    tri = jnp.where(tri, 1.0, 0.0).astype(bf16)
    hot = jnp.concatenate([
        jnp.where(lax.broadcasted_iota(i32, (groups, sampled), 0) == owner[k], 1.0, 0.0)
        for k in range(kinds)], axis=0)
    lines = kinds * groups
    pieces = [hot[:, base:base + STEP] for base in range(0, sampled, STEP)]
    upto = jnp.dot(jnp.concatenate(pieces, axis=0).astype(bf16), tri, preferred_element_type=f32)
    carry = jnp.zeros((lines, 1), f32)
    ranks = []
    for n, piece in enumerate(pieces):
        here = upto[n * lines:(n + 1) * lines]
        ranks.append((here + (carry - 1.0)) * piece)
        carry = carry + here[:, STEP - 1:]
    ranks = jnp.concatenate(ranks, axis=1)

    blocks = sampled // LANES
    parts = cap // LANES
    for k in range(kinds):
        mine = hot[k * groups:(k + 1) * groups]
        rank = jnp.sum(ranks[k * groups:(k + 1) * groups], axis=0, keepdims=True).astype(i32)
        place = owner[k] * cap + rank
        coarse = (place >> 8).astype(f32)
        fine = (place & 255).astype(f32)
        table[k] = jnp.concatenate(
            [part[:, b * LANES:(b + 1) * LANES] for part in (coarse, fine) for b in range(blocks)], axis=0).astype(bf16)
        wanted = row[k:k + 1, :]
        tall = mine * (wanted >> 8).astype(f32)
        wide = mine * (wanted & 255).astype(f32)
        bank = rank >> log2(LANES)
        stack = jnp.concatenate(
            [jnp.where(bank == h, part, 0.0) for part in (tall, wide) for h in range(parts)], axis=0).astype(bf16)
        listed = lax.dot_general(stack, hits(rank & (LANES - 1), LANES), NT, preferred_element_type=f32)
        listed = (listed[:parts * groups] * 256.0 + listed[parts * groups:]).astype(i32)
        seeds = jnp.where(mine[:, :SEEDS] > 0.0, rank[:, :SEEDS], -1)
        for o in range(groups):
            for h in range(parts):
                req_send[o, k:k + 1, h * LANES:(h + 1) * LANES] = listed[h * groups + o:h * groups + o + 1]
            req_send[o, k:k + 1, cap:] = seeds[o:o + 1]

    def order(i):
        return i + 2 if i < items - 2 else items - 1 - i

    def request_copy(t):
        to = g ^ (CORES * t + core)
        return remote(req_send.at[to], req_recv.at[t], req_ss.at[t], req_rs.at[t], to, m)

    for i in range(items):
        t = order(i)
        if t == 0:
            @pl.when(core > 0)
            def _():
                request_copy(0).start()

            @pl.when(core == 0)
            def _():
                req_recv[0] = req_send[g]
        else:
            request_copy(t).start()

    slots = lax.broadcasted_iota(i32, (1, edge_total), 1)
    banks = lax.broadcasted_iota(i32, (blocks, edge_total), 0)
    ones8 = jnp.ones((8, LANES), bf16)
    for j in range(SHARE):
        r = core * SHARE + j
        kind = RELATION_SOURCE[j] + core * (RELATION_SOURCE[SHARE + j] - RELATION_SOURCE[j])
        wanted = src[pl.ds(r, 1), :]
        found = jnp.dot(table[kind], hits(wanted & (LANES - 1), LANES), preferred_element_type=f32)
        found = found[:blocks] * 256.0 + found[blocks:]
        found = jnp.where(banks == (wanted >> log2(LANES)), found, 0.0)
        place = jnp.sum(found, axis=0, keepdims=True).astype(i32)
        live = slots < count[0, r]
        ends = dst[pl.ds(r, 1), :]
        info_send[j:j + 1, :edge_total] = jnp.where(live, place * SEEDS + ends, -1)
        marks = hits(jnp.where(live, ends, -1), SEEDS)
        tally = marks[:, :LANES]
        for base in range(LANES, edge_total, LANES):
            tally = tally + marks[:, base:base + LANES]
        tally = lax.dot_general(ones8, tally, NT, preferred_element_type=f32)
        info_send[j:j + 1, edge_total:] = tally[:1].astype(i32)

    def info_copy(d):
        return remote(info_send, info_recv.at[d // CORES, core], info_ss.at[d], info_rs.at[d // CORES, core],
                      g ^ d, plane * CORES + d % CORES)

    for i in range(items):
        for c in reversed(range(CORES)):
            d = CORES * order(i) + c
            if d == 0:
                @pl.when(core > 0)
                def _():
                    info_copy(0).start()

                @pl.when(core == 0)
                def _():
                    info_recv[0, 0] = info_send[...]
            else:
                info_copy(d).start()

    def info_wait(t, c):
        remote(info_send, info_recv.at[t, c], info_ss.at[0], info_rs.at[t, c], g, mate).wait_recv()

    def x_copy(i, w, e, t=slice(None)):
        to = lax.rem(plane + e, planes) * CORES + core
        return remote(xsend.at[i, t, w, e], xrecv.at[i, t, w, e], x_ss.at[i, w, e - 1], x_rs.at[i, w, e - 1], g, to)

    def y_copy(i, t=slice(None)):
        return remote(xsend.at[i, t, 1], yrecv.at[i, t], y_ss.at[i], y_rs.at[i], g ^ 1, plane * CORES)

    def z_copy(i, d, w, c, t):
        return remote(zsend.at[i, t, w, c], zrecv.at[d, t, w], z_ss.at[i, w], z_rs.at[d, w],
                      g ^ d, plane * CORES + c)

    near = items - 2

    def side(e):
        return CORES * order(near) if e == 0 else groups + (planes - 1) * CORES + e - 1

    def near_copy(e, c):
        return remote(xsend.at[near, :, 1, e, c], zrecv.at[side(e), :, 1], near_ss.at[e, c], near_rs.at[e],
                      g ^ (CORES * order(near)), lax.rem(plane + e, planes) * CORES + c)

    def z_sent(i, w):
        return remote(zsend.at[i, :, w], zsend.at[i, :, w], z_ss.at[i, w], z_rs.at[0, w], g, mate)

    def z_landed(d, w):
        return remote(zrecv.at[d, :, w], zrecv.at[d, :, w], z_ss.at[0, w], z_rs.at[d, w], g, mate)

    def far(e, d):
        return d if e == 0 else groups + (e - 1) * CORES + d

    def own_copy(e, c, d, t=slice(None)):
        return remote(xsend.at[items - 1, t, :, e, c], zrecv.at[far(e, d), t], own_ss.at[e, c], own_rs.at[e, d],
                      g ^ d, lax.rem(plane + e, planes) * CORES + c)

    def spot(i):
        return jnp.where(i < items - 2, i + 2, items - 1 - i)

    def merge(i):
        y_copy(i).wait_recv()
        for n in range(kinds):
            for e in range(planes):
                for c in range(CORES):
                    total = xsend[i, n, 1, e, c].astype(f32) + yrecv[i, n, e, c].astype(f32)
                    xsend[i, n, 1, e, c] = total.astype(bf16)
        for e in reversed(range(planes)):
            if isinstance(i, int) and i == near:
                for c in range(CORES):
                    near_copy(e, c).start()
            elif e:
                x_copy(i, 1, e).start()

    def deliver(i, w):
        d = CORES * spot(i) + core
        for e in range(1, planes):
            x_copy(i, w, e).wait_recv()
        for n in range(kinds):
            for c in range(CORES):
                total = xsend[i, n, w, 0, c].astype(f32)
                for e in range(1, planes):
                    total = total + xrecv[i, n, w, e, c].astype(f32)
                zsend[i, n, w, c] = total.astype(bf16)
        for c in range(CORES):
            z_copy(i, d, w, c, slice(None)).start()

    def pick(t, where, sides):
        tall = len(sides) * feat
        for k in range(kinds):
            wanted = req_recv[t, k:k + 1, :cap]
            bank = wanted >> log2(low)
            fine = wanted & (low - 1)
            choice = jnp.concatenate(
                [hits(jnp.where((fine >= base) & (fine < base + STEP), fine - base, -1), STEP)
                 for base in range(0, low, STEP)], axis=0)
            rows_k = jnp.concatenate(
                [feats[k, c, :, h * low:(h + 1) * low] for h in range(high) for c in sides], axis=0)
            found = jnp.dot(rows_k, choice, preferred_element_type=f32)
            chosen = found[:tall]
            for h in range(1, high):
                chosen = jnp.where(bank == h, found[h * tall:(h + 1) * tall], chosen)
            picked[where, k, :, sides[0] * feat:(sides[-1] + 1) * feat] = chosen.astype(bf16).T

    def build(place, ref_l, ref_r, n, width):
        left = hits(ref_l[n:n + 1, :width], lo_n, ONE_HOT)
        right = hits(ref_r[n:n + 1, :width], hi_n * SEEDS, ONE_HOT)
        counts = lax.dot_general(right, left, NT, preferred_element_type=f32).astype(bf16)
        for h in range(hi_n):
            adj[place, :, h * lo_n:(h + 1) * lo_n] = counts[h * SEEDS:(h + 1) * SEEDS]

    def item(i, first, last):
        t = order(i) if first or last else spot(i)
        where = 1 if last else 0
        if first:
            request_copy(t).wait_recv()
            pick(t, 0, range(CORES))
            for c in range(CORES):
                info_wait(t, c)
            loads[kinds].wait()
            swaps[kinds].wait()
        if not first and not last:
            pick(t, 0, range(CORES))
        for c in range(CORES):
            packed = info_recv[t, c, :, :edge_total] - g * (cap * SEEDS)
            ok = (packed >= 0) & (packed < cap * SEEDS)
            slot = packed >> log2(SEEDS)
            lidx[c * SHARE:(c + 1) * SHARE, :] = (slot & (lo_n - 1)).astype(f32)
            ridx[c * SHARE:(c + 1) * SHARE, :] = jnp.where(
                ok, (slot >> log2(lo_n)) * SEEDS + (packed & (SEEDS - 1)), -1).astype(f32)
        slot = req_recv[t, :, cap:]
        lidx[RELS:RELS + kinds, :SEEDS] = (slot & (lo_n - 1)).astype(f32)
        ridx[RELS:RELS + kinds, :SEEDS] = jnp.where(
            slot >= 0, (slot >> log2(lo_n)) * SEEDS + lax.broadcasted_iota(i32, slot.shape, 1), -1).astype(f32)
        degree = jnp.concatenate([info_recv[t, c, :, edge_total:] for c in range(CORES)], axis=0)
        inverse = (1.0 / jnp.maximum(degree.astype(f32), 1.0)).T
        groups_of = [[matrix for matrix in range(MATS) if MATRIX_TARGET[matrix] == n] for n in range(kinds)]

        def make(matrix):
            build(matrix, lidx, ridx, matrix, edge_total if matrix < RELS else SEEDS)

        def gather(n):
            values = []
            for matrix in groups_of[n]:
                kind = RELATION_SOURCE[matrix] if matrix < RELS else matrix - RELS
                value = jnp.dot(adj[matrix], picked[where, kind], preferred_element_type=f32)
                if matrix < RELS:
                    value = value * inverse[:, matrix:matrix + 1]
                values.append(value.astype(bf16))
            return jnp.concatenate(values, axis=1)

        def emit(n, left):
            right = jnp.concatenate([weights[c, matrix] for matrix in groups_of[n] for c in range(CORES)], axis=0)
            typed = jnp.dot(left, right, preferred_element_type=f32).astype(bf16)
            for p in range(planes):
                for w in range(WAYS):
                    for c in range(CORES):
                        xsend[i, n, w, lax.rem(p - plane + planes, planes), c] = typed[
                            w * span:(w + 1) * span, p * half + c * quarter:p * half + (c + 1) * quarter]
            if last:
                for e in reversed(range(planes)):
                    for c in range(CORES):
                        if e or c:
                            own_copy(e, c, core, n).start()

                @pl.when(core > 0)
                def _():
                    own_copy(0, 0, core, n).start()

                @pl.when(core == 0)
                def _():
                    for w in range(WAYS):
                        zrecv[0, n, w] = xsend[i, n, w, 0, 0]
            else:
                for e in range(1, planes):
                    x_copy(i, 0, e, n).start()

                @pl.when(core > 0)
                def _():
                    y_copy(i, n).start()

        for matrix in groups_of[0] + groups_of[1][:1]:
            make(matrix)
        left = gather(0)
        make(groups_of[1][1])
        emit(0, left)
        def relay():
            @pl.when((i >= 2) & (core == 0))
            def _():
                deliver(i - 2, 1)

        def advance():
            relay()

            @pl.when(core == 0)
            def _():
                merge(i - 1)

            deliver(i - 1, 0)

        if not first and not last:
            advance()
        for matrix in groups_of[1][2:] + groups_of[2][:1]:
            make(matrix)
        left = gather(1)
        for matrix in groups_of[2][1:]:
            make(matrix)
        emit(1, left)
        if last:
            advance()
        emit(2, gather(2))

    def rest(i, _):
        item(i, False, False)
        return 0

    for k in range(kinds):
        loads[k].wait()

    @pl.when(core > 0)
    def _():
        request_copy(0).wait_recv()
    pick(0, 1, (0,))
    for k in range(kinds):
        swaps[k].wait()
    pick(0, 1, (1,))
    item(0, True, False)
    for i in range(1, items - 1):
        request_copy(order(i)).wait_recv()
        for c in range(CORES):
            info_wait(order(i), c)
    info_wait(0, 1)

    @pl.when(core > 0)
    def _():
        info_wait(0, 0)
    lax.fori_loop(1, items - 1, rest, 0)
    item(items - 1, False, True)

    pieces = []
    for i in range(items - 1):
        for w in range(WAYS):
            for c in range(CORES if w == 0 else 1):
                d = CORES * order(i) + c
                if w == 0 or i < near:
                    z_landed(d, w).wait_recv()
                    pieces.append((w, d))
    for e in range(planes):
        near_copy(e, 0).wait_recv()
        pieces.append((1, side(e)))
    for e in range(planes):
        for d in range(CORES):
            if e or d:
                own_copy(e, 0, d).wait_recv()
            else:
                @pl.when(core > 0)
                def _():
                    own_copy(0, 0, 0).wait_recv()
            for w in range(WAYS):
                pieces.append((w, far(e, d)))
    for n in range(kinds):
        halves = []
        for w in range(WAYS):
            total = jnp.zeros((span, quarter), f32)
            for v, place in pieces:
                if v == w:
                    total = total + zrecv[place, n, w].astype(f32)
            halves.append(total)
        out[n] = jnp.maximum(jnp.concatenate(halves, axis=0), 0.0).T.astype(bf16)
    for t in range(items):
        if t == 0:
            @pl.when(core > 0)
            def _():
                request_copy(0).wait_send()
                info_copy(0).wait_send()
        else:
            request_copy(t).wait_send()
            info_copy(CORES * t).wait_send()
        for c in range(1, CORES):
            info_copy(CORES * t + c).wait_send()
    for i in range(items - 1):
        for e in range(1, planes):
            x_copy(i, 0, e).wait_send()
        z_sent(i, 0).wait_send()

        @pl.when(core == 0)
        def _():
            if i < near:
                for e in range(1, planes):
                    x_copy(i, 1, e).wait_send()
                z_sent(i, 1).wait_send()
            else:
                for e in range(planes):
                    for c in range(CORES):
                        near_copy(e, c).wait_send()

        @pl.when(core > 0)
        def _():
            y_copy(i).wait_send()
    for e in range(planes):
        for c in range(CORES):
            if e or c:
                own_copy(e, c, core).wait_send()

    @pl.when(core > 0)
    def _():
        own_copy(0, 0, core).wait_send()


def per_device(features, weights, sample_owner, sample_row, edge_src, edge_dst, edge_count):
    groups, shares = lax.axis_size("dp"), lax.axis_size("mp")
    kinds, feat, rows = features.shape
    sampled, edge_total = sample_row.shape[1], edge_src.shape[1]
    cap = 2 * sampled // groups
    items, planes = groups // CORES, shares // CORES
    width = weights.shape[2]
    quarter = width // shares
    bf16, f32, i32 = jnp.bfloat16, jnp.float32, jnp.int32
    vmem = pl.BlockSpec(memory_space=pltpu.VMEM)
    hbm = pl.BlockSpec(memory_space=pltpu.HBM)
    dma = pltpu.SemaphoreType.DMA
    return pl.pallas_call(
        functools.partial(kernel, groups, shares),
        out_shape=jax.ShapeDtypeStruct((kinds, quarter, SEEDS), bf16),
        in_specs=[hbm] * 7,
        out_specs=vmem,
        scratch_shapes=[
            pltpu.VMEM((kinds, 1, sampled), i32),
            pltpu.VMEM((kinds, sampled), i32),
            pltpu.VMEM(edge_src.shape, i32),
            pltpu.VMEM(edge_src.shape, i32),
            pltpu.SMEM((1, RELS), i32),
            pltpu.VMEM((kinds, CORES, feat, rows), bf16),
            pltpu.VMEM((CORES, MATS, feat, width), bf16),
            pltpu.VMEM((groups, kinds, cap + SEEDS), i32),
            pltpu.VMEM((items, kinds, cap + SEEDS), i32),
            pltpu.VMEM((SHARE, edge_total + SEEDS), i32),
            pltpu.VMEM((items, CORES, SHARE, edge_total + SEEDS), i32),
            pltpu.VMEM((kinds, 2 * sampled // LANES, LANES), bf16),
            pltpu.VMEM((16, edge_total), f32),
            pltpu.VMEM((16, edge_total), f32),
            pltpu.VMEM((2, kinds, cap, CORES * feat), bf16),
            pltpu.VMEM((MATS, SEEDS, cap), bf16),
            pltpu.VMEM((items, kinds, WAYS, planes, CORES, SEEDS // WAYS, quarter), bf16),
            pltpu.VMEM((items, kinds, WAYS, planes, CORES, SEEDS // WAYS, quarter), bf16),
            pltpu.VMEM((items, kinds, planes, CORES, SEEDS // WAYS, quarter), bf16),
            pltpu.VMEM((items, kinds, WAYS, CORES, SEEDS // WAYS, quarter), bf16),
            pltpu.VMEM((groups + (planes - 1) * (CORES + 1), kinds, WAYS, SEEDS // WAYS, quarter), bf16),
            dma((kinds + 1,)), dma((5,)), dma((kinds + 1,)), dma((kinds + 1,)),
            dma((items,)), dma((items,)),
            dma((groups,)), dma((items, CORES)),
            dma((items - 1, WAYS, planes - 1)), dma((items - 1, WAYS, planes - 1)),
            dma((items - 1,)), dma((items - 1,)),
            dma((items - 1, WAYS)), dma((groups, WAYS)),
            dma((planes, CORES)), dma((planes, CORES)),
            dma((planes, CORES)), dma((planes,)),
        ],
        compiler_params=pltpu.CompilerParams(
            collective_id=0, has_side_effects=True, vmem_limit_bytes=48 * 1024 * 1024),
    )(*[pltpu.with_memory_space_constraint(value, pltpu.HBM) for value in (
        features, weights, sample_owner.transpose(0, 2, 1), sample_row, edge_src, edge_dst, edge_count.T)])


def solution(mesh):
    return jax.shard_map(
        per_device,
        mesh=mesh,
        in_specs=(
            P(None, "mp", "dp"),
            P(None, "mp", None),
            P(None, "dp", None),
            P(None, "dp"),
            P(None, "dp"),
            P(None, "dp"),
            P(None, "dp"),
        ),
        out_specs=P(None, "mp", "dp"),
        check_vma=False,
    )
```

```python
import functools

import jax
import jax.numpy as jnp
from jax import lax
from jax.experimental import pallas as pl
from jax.experimental.pallas import tpu as pltpu
from jax.sharding import PartitionSpec as P

SEEDS = 128
RELATION_SOURCE = (0, 1, 0, 1, 2, 0, 2, 1)
MATRIX_TARGET = (1, 0, 0, 2, 1, 2, 0, 1, 0, 1, 2)
RELS = len(RELATION_SOURCE)
KINDS = 3
MATS = RELS + KINDS
SLOTS = tuple(
    tuple([r for r in range(RELS) if RELATION_SOURCE[r] == k] + [RELS + k]) for k in range(KINDS)
)
ORDER = tuple(m for group in SLOTS for m in group)
STARTS = tuple(sum(len(group) for group in SLOTS[:k]) for k in range(KINDS))
PLACE = tuple(ORDER.index(m) for m in range(MATS))
CORES = 2
WAYS = 2
SHARE = RELS // CORES
STEP = 256
LANES = 128
ONE_HOT = jnp.float8_e4m3fn
MESH = pl.DeviceIdType.MESH
NT = (((1,), (1,)), ((), ()))


def log2(n):
    return n.bit_length() - 1


def kernel(groups, shares, features_in, weights_in, owner_in, row_in, src_in, dst_in, count_in, out,
           owner, row, src, dst, count, feats, weights, req_send, req_recv, info_send, info_recv, table,
           lidx, ridx, picked, adj, xsend, xrecv, yrecv, zsend, zrecv,
           in_sem, list_sem, fx_ss, fx_rs, req_ss, req_rs, info_ss, info_rs, x_ss, x_rs, y_ss, y_rs, z_ss, z_rs, own_ss, own_rs, near_ss, near_rs):
    kinds, _, feat, rows = feats.shape
    both = CORES * feat
    sampled = row.shape[1]
    edge_total = src.shape[1]
    cap = req_send.shape[2] - SEEDS
    low = min(512, rows)
    high = rows // low
    lo_n = min(STEP, cap)
    hi_n = cap // lo_n
    items = groups // CORES
    planes = shares // CORES
    quarter = xsend.shape[6]
    span = SEEDS // WAYS
    half = CORES * quarter
    g = lax.axis_index("dp")
    m = lax.axis_index("mp")
    core = lax.rem(m, CORES)
    plane = m // CORES
    f32, bf16, i32 = jnp.float32, jnp.bfloat16, jnp.int32

    def at(group, mp):
        return {"dp": group, "mp": mp}

    def remote(source, target, ss, rs, group, mp):
        return pltpu.make_async_remote_copy(source, target, ss, rs, device_id=at(group, mp), device_id_type=MESH)

    def levels(size):
        return lax.broadcasted_iota(i32, (size, LANES), 0).astype(f32).astype(bf16)

    def hits(index, size, kind=bf16):
        level = levels(size)
        index = index.astype(f32).astype(bf16)
        yes, no = jnp.ones((), kind), jnp.zeros((), kind)
        return jnp.concatenate(
            [jnp.where(level == index[:, base:base + LANES], yes, no)
             for base in range(0, index.shape[1], LANES)], axis=1)

    mate = m - core + lax.rem(core + 1, CORES)
    loads, swaps = [], []
    for k in range(kinds):
        loads.append(pltpu.make_async_copy(features_in.at[k], feats.at[k, 0], in_sem.at[k]))
        swaps.append(remote(feats.at[k, 0], feats.at[k, 1], fx_ss.at[k], fx_rs.at[k], g, mate))
    loads.append(pltpu.make_async_copy(weights_in, weights.at[0], in_sem.at[kinds]))
    swaps.append(remote(weights.at[0], weights.at[1], fx_ss.at[kinds], fx_rs.at[kinds], g, mate))
    lists = [pltpu.make_async_copy(source, target, list_sem.at[n]) for n, (source, target) in enumerate(
        ((owner_in, owner), (row_in, row), (src_in, src), (dst_in, dst), (count_in, count)))]
    for copy in lists + loads:
        copy.start()

    barrier = pltpu.get_barrier_semaphore()
    pl.semaphore_signal(barrier, inc=1, device_id=at(g, mate), device_id_type=MESH)
    for d in range(1, groups):
        for c in range(CORES):
            pl.semaphore_signal(barrier, inc=1, device_id=at(g ^ d, plane * CORES + c), device_id_type=MESH)
    for e in range(1, planes):
        pl.semaphore_signal(
            barrier, inc=1, device_id=at(g, lax.rem(plane + e, planes) * CORES + core), device_id_type=MESH)
    for copy in lists:
        copy.wait()

    tri = (lax.broadcasted_iota(i32, (STEP, STEP), 0) <= lax.broadcasted_iota(i32, (STEP, STEP), 1))
    tri = jnp.where(tri, 1.0, 0.0).astype(bf16)
    hot = jnp.concatenate([
        jnp.where(lax.broadcasted_iota(i32, (groups, sampled), 0) == owner[k], 1.0, 0.0)
        for k in range(kinds)], axis=0)
    lines = kinds * groups
    pieces = [hot[:, base:base + STEP] for base in range(0, sampled, STEP)]
    upto = jnp.dot(jnp.concatenate(pieces, axis=0).astype(bf16), tri, preferred_element_type=f32)
    carry = jnp.zeros((lines, 1), f32)
    ranks = []
    for n, piece in enumerate(pieces):
        here = upto[n * lines:(n + 1) * lines]
        ranks.append((here + (carry - 1.0)) * piece)
        carry = carry + here[:, STEP - 1:]
    ranks = jnp.concatenate(ranks, axis=1)

    blocks = sampled // LANES
    parts = cap // LANES
    places = []
    for k in range(kinds):
        mine = hot[k * groups:(k + 1) * groups]
        rank = jnp.sum(ranks[k * groups:(k + 1) * groups], axis=0, keepdims=True).astype(i32)
        places.append(owner[k] * cap + rank)
        wanted = row[k:k + 1, :]
        tall = mine * (wanted >> 8).astype(f32)
        wide = mine * (wanted & 255).astype(f32)
        bank = rank >> log2(LANES)
        stack = jnp.concatenate(
            [jnp.where(bank == h, part, 0.0) for part in (tall, wide) for h in range(parts)], axis=0).astype(bf16)
        listed = lax.dot_general(stack, hits(rank & (LANES - 1), LANES), NT, preferred_element_type=f32)
        listed = (listed[:parts * groups] * 256.0 + listed[parts * groups:]).astype(i32)
        seeds = jnp.where(mine[:, :SEEDS] > 0.0, rank[:, :SEEDS], -1)
        for o in range(groups):
            for h in range(parts):
                req_send[o, k:k + 1, h * LANES:(h + 1) * LANES] = listed[h * groups + o:h * groups + o + 1]
            req_send[o, k:k + 1, cap:] = seeds[o:o + 1]

    for copy in loads:
        copy.wait()
    pl.semaphore_wait(barrier, CORES * (groups - 1) + planes)
    for copy in swaps:
        copy.start()

    def order(i):
        return i + 2 if i < items - 2 else items - 1 - i

    def request_copy(t):
        to = g ^ (CORES * t + core)
        return remote(req_send.at[to], req_recv.at[t], req_ss.at[t], req_rs.at[t], to, m)

    for i in range(items):
        t = order(i)
        if t == 0:
            @pl.when(core > 0)
            def _():
                request_copy(0).start()

            @pl.when(core == 0)
            def _():
                req_recv[0] = req_send[g]
        else:
            request_copy(t).start()

    for k in range(kinds):
        coarse = (places[k] >> 8).astype(f32)
        fine = (places[k] & 255).astype(f32)
        table[k] = jnp.concatenate(
            [part[:, b * LANES:(b + 1) * LANES] for part in (coarse, fine) for b in range(blocks)], axis=0).astype(bf16)
    slots = lax.broadcasted_iota(i32, (1, edge_total), 1)
    banks = lax.broadcasted_iota(i32, (blocks, edge_total), 0)
    ones8 = jnp.ones((8, LANES), bf16)
    for j in range(SHARE):
        r = core * SHARE + j
        kind = RELATION_SOURCE[j] + core * (RELATION_SOURCE[SHARE + j] - RELATION_SOURCE[j])
        wanted = src[pl.ds(r, 1), :]
        found = jnp.dot(table[kind], hits(wanted & (LANES - 1), LANES), preferred_element_type=f32)
        found = found[:blocks] * 256.0 + found[blocks:]
        found = jnp.where(banks == (wanted >> log2(LANES)), found, 0.0)
        place = jnp.sum(found, axis=0, keepdims=True).astype(i32)
        live = slots < count[0, r]
        ends = dst[pl.ds(r, 1), :]
        info_send[j:j + 1, :edge_total] = jnp.where(live, place * SEEDS + ends, -1)
        marks = hits(jnp.where(live, ends, -1), SEEDS)
        tally = marks[:, :LANES]
        for base in range(LANES, edge_total, LANES):
            tally = tally + marks[:, base:base + LANES]
        tally = lax.dot_general(ones8, tally, NT, preferred_element_type=f32)
        info_send[j:j + 1, edge_total:] = tally[:1].astype(i32)

    def info_copy(d):
        return remote(info_send, info_recv.at[d // CORES, core], info_ss.at[d], info_rs.at[d // CORES, core],
                      g ^ d, plane * CORES + d % CORES)

    for i in range(items):
        for c in reversed(range(CORES)):
            d = CORES * order(i) + c
            if d == 0:
                @pl.when(core > 0)
                def _():
                    info_copy(0).start()

                @pl.when(core == 0)
                def _():
                    info_recv[0, 0] = info_send[...]
            else:
                info_copy(d).start()

    def info_wait(t, c):
        remote(info_send, info_recv.at[t, c], info_ss.at[0], info_rs.at[t, c], g, mate).wait_recv()

    def x_copy(i, w, e, t=slice(None)):
        to = lax.rem(plane + e, planes) * CORES + core
        return remote(xsend.at[i, t, w, e], xrecv.at[i, t, w, e], x_ss.at[i, w, e - 1], x_rs.at[i, w, e - 1], g, to)

    def y_copy(i, t=slice(None)):
        return remote(xsend.at[i, t, 1], yrecv.at[i, t], y_ss.at[i], y_rs.at[i], g ^ 1, plane * CORES)

    def z_copy(i, d, w, c, t):
        return remote(zsend.at[i, t, w, c], zrecv.at[d, t, w], z_ss.at[i, w], z_rs.at[d, w],
                      g ^ d, plane * CORES + c)

    near = items - 2

    def side(e):
        return CORES * order(near) if e == 0 else groups + (planes - 1) * CORES + e - 1

    def near_copy(e, c):
        return remote(xsend.at[near, :, 1, e, c], zrecv.at[side(e), :, 1], near_ss.at[e, c], near_rs.at[e],
                      g ^ (CORES * order(near)), lax.rem(plane + e, planes) * CORES + c)

    def z_sent(i, w):
        return remote(zsend.at[i, :, w], zsend.at[i, :, w], z_ss.at[i, w], z_rs.at[0, w], g, mate)

    def z_landed(d, w):
        return remote(zrecv.at[d, :, w], zrecv.at[d, :, w], z_ss.at[0, w], z_rs.at[d, w], g, mate)

    def far(e, d):
        return d if e == 0 else groups + (e - 1) * CORES + d

    def own_copy(e, c, d, t=slice(None)):
        return remote(xsend.at[items - 1, t, :, e, c], zrecv.at[far(e, d), t], own_ss.at[e, c], own_rs.at[e, d],
                      g ^ d, lax.rem(plane + e, planes) * CORES + c)

    def spot(i):
        return jnp.where(i < items - 2, i + 2, items - 1 - i)

    def merge(i):
        y_copy(i).wait_recv()
        for n in range(kinds):
            for e in range(planes):
                for c in range(CORES):
                    total = xsend[i, n, 1, e, c].astype(f32) + yrecv[i, n, e, c].astype(f32)
                    xsend[i, n, 1, e, c] = total.astype(bf16)
        for e in reversed(range(planes)):
            if isinstance(i, int) and i == near:
                for c in range(CORES):
                    near_copy(e, c).start()
            elif e:
                x_copy(i, 1, e).start()

    def deliver(i, w):
        d = CORES * spot(i) + core
        for e in range(1, planes):
            x_copy(i, w, e).wait_recv()
        for n in range(kinds):
            for c in range(CORES):
                total = xsend[i, n, w, 0, c].astype(f32)
                for e in range(1, planes):
                    total = total + xrecv[i, n, w, e, c].astype(f32)
                zsend[i, n, w, c] = total.astype(bf16)
        for c in range(CORES):
            z_copy(i, d, w, c, slice(None)).start()

    def pick(t, where, sides):
        tall = len(sides) * feat
        for k in range(kinds):
            wanted = req_recv[t, k:k + 1, :cap]
            bank = wanted >> log2(low)
            fine = wanted & (low - 1)
            choice = jnp.concatenate(
                [hits(jnp.where((fine >= base) & (fine < base + STEP), fine - base, -1), STEP)
                 for base in range(0, low, STEP)], axis=0)
            rows_k = jnp.concatenate(
                [feats[k, c, :, h * low:(h + 1) * low] for h in range(high) for c in sides], axis=0)
            found = jnp.dot(rows_k, choice, preferred_element_type=f32)
            chosen = found[:tall]
            for h in range(1, high):
                chosen = jnp.where(bank == h, found[h * tall:(h + 1) * tall], chosen)
            picked[where, k, :, sides[0] * feat:(sides[-1] + 1) * feat] = chosen.astype(bf16).T

    def build(place, ref_l, ref_r, n, width):
        left = hits(ref_l[n:n + 1, :width], lo_n, ONE_HOT)
        right = hits(ref_r[n:n + 1, :width], hi_n * SEEDS, ONE_HOT)
        counts = lax.dot_general(right, left, NT, preferred_element_type=f32).astype(bf16)
        for h in range(hi_n):
            adj[place, :, h * lo_n:(h + 1) * lo_n] = counts[h * SEEDS:(h + 1) * SEEDS]

    def item(i, first, last):
        t = order(i) if first or last else spot(i)
        where = 1 if last else 0
        if first:
            request_copy(t).wait_recv()
            pick(t, 0, range(CORES))
            for c in range(CORES):
                info_wait(t, c)
            swaps[kinds].wait()
        if not first and not last:
            pick(t, 0, range(CORES))
        for c in range(CORES):
            packed = info_recv[t, c, :, :edge_total] - g * (cap * SEEDS)
            ok = (packed >= 0) & (packed < cap * SEEDS)
            slot = packed >> log2(SEEDS)
            lidx[c * SHARE:(c + 1) * SHARE, :] = (slot & (lo_n - 1)).astype(f32)
            ridx[c * SHARE:(c + 1) * SHARE, :] = jnp.where(
                ok, (slot >> log2(lo_n)) * SEEDS + (packed & (SEEDS - 1)), -1).astype(f32)
        slot = req_recv[t, :, cap:]
        lidx[RELS:RELS + kinds, :SEEDS] = (slot & (lo_n - 1)).astype(f32)
        ridx[RELS:RELS + kinds, :SEEDS] = jnp.where(
            slot >= 0, (slot >> log2(lo_n)) * SEEDS + lax.broadcasted_iota(i32, slot.shape, 1), -1).astype(f32)
        degree = jnp.concatenate([info_recv[t, c, :, edge_total:] for c in range(CORES)], axis=0)
        inverse = (1.0 / jnp.maximum(degree.astype(f32), 1.0)).T
        groups_of = [[matrix for matrix in range(MATS) if MATRIX_TARGET[matrix] == n] for n in range(kinds)]

        def make(matrix):
            build(matrix, lidx, ridx, matrix, edge_total if matrix < RELS else SEEDS)

        def gather(n):
            values = []
            for matrix in groups_of[n]:
                kind = RELATION_SOURCE[matrix] if matrix < RELS else matrix - RELS
                value = jnp.dot(adj[matrix], picked[where, kind], preferred_element_type=f32)
                if matrix < RELS:
                    value = value * inverse[:, matrix:matrix + 1]
                values.append(value.astype(bf16))
            return jnp.concatenate(values, axis=1)

        def emit(n, left):
            right = jnp.concatenate([weights[c, matrix] for matrix in groups_of[n] for c in range(CORES)], axis=0)
            typed = jnp.dot(left, right, preferred_element_type=f32).astype(bf16)
            for p in range(planes):
                for w in range(WAYS):
                    for c in range(CORES):
                        xsend[i, n, w, lax.rem(p - plane + planes, planes), c] = typed[
                            w * span:(w + 1) * span, p * half + c * quarter:p * half + (c + 1) * quarter]
            if last:
                for e in reversed(range(planes)):
                    for c in range(CORES):
                        if e or c:
                            own_copy(e, c, core, n).start()

                @pl.when(core > 0)
                def _():
                    own_copy(0, 0, core, n).start()

                @pl.when(core == 0)
                def _():
                    for w in range(WAYS):
                        zrecv[0, n, w] = xsend[i, n, w, 0, 0]
            else:
                for e in range(1, planes):
                    x_copy(i, 0, e, n).start()

                @pl.when(core > 0)
                def _():
                    y_copy(i, n).start()

        for matrix in groups_of[0] + groups_of[1][:1]:
            make(matrix)
        left = gather(0)
        make(groups_of[1][1])
        emit(0, left)
        def relay():
            @pl.when((i >= 2) & (core == 0))
            def _():
                deliver(i - 2, 1)

        def advance():
            relay()

            @pl.when(core == 0)
            def _():
                merge(i - 1)

            deliver(i - 1, 0)

        if not first and not last:
            advance()
        for matrix in groups_of[1][2:] + groups_of[2][:1]:
            make(matrix)
        left = gather(1)
        for matrix in groups_of[2][1:]:
            make(matrix)
        emit(1, left)
        emit(2, gather(2))
        if last:
            advance()

    def rest(i, _):
        item(i, False, False)
        return 0

    @pl.when(core > 0)
    def _():
        request_copy(0).wait_recv()
    pick(0, 1, (0,))
    for k in range(kinds):
        swaps[k].wait()
    pick(0, 1, (1,))
    item(0, True, False)
    for i in range(1, items - 1):
        request_copy(order(i)).wait_recv()
        for c in range(CORES):
            info_wait(order(i), c)
    info_wait(0, 1)

    @pl.when(core > 0)
    def _():
        info_wait(0, 0)
    lax.fori_loop(1, items - 1, rest, 0)
    item(items - 1, False, True)

    pieces = []
    for i in range(items - 1):
        for w in range(WAYS):
            for c in range(CORES if w == 0 else 1):
                d = CORES * order(i) + c
                if w == 0 or i < near:
                    z_landed(d, w).wait_recv()
                    pieces.append((w, d))
    for e in range(planes):
        near_copy(e, 0).wait_recv()
        pieces.append((1, side(e)))
    for e in range(planes):
        for d in range(CORES):
            if e or d:
                own_copy(e, 0, d).wait_recv()
            else:
                @pl.when(core > 0)
                def _():
                    own_copy(0, 0, 0).wait_recv()
            for w in range(WAYS):
                pieces.append((w, far(e, d)))
    for n in range(kinds):
        halves = []
        for w in range(WAYS):
            total = jnp.zeros((span, quarter), f32)
            for v, place in pieces:
                if v == w:
                    total = total + zrecv[place, n, w].astype(f32)
            halves.append(total)
        out[n] = jnp.maximum(jnp.concatenate(halves, axis=0), 0.0).T.astype(bf16)
    for t in range(items):
        if t == 0:
            @pl.when(core > 0)
            def _():
                request_copy(0).wait_send()
                info_copy(0).wait_send()
        else:
            request_copy(t).wait_send()
            info_copy(CORES * t).wait_send()
        for c in range(1, CORES):
            info_copy(CORES * t + c).wait_send()
    for i in range(items - 1):
        for e in range(1, planes):
            x_copy(i, 0, e).wait_send()
        z_sent(i, 0).wait_send()

        @pl.when(core == 0)
        def _():
            if i < near:
                for e in range(1, planes):
                    x_copy(i, 1, e).wait_send()
                z_sent(i, 1).wait_send()
            else:
                for e in range(planes):
                    for c in range(CORES):
                        near_copy(e, c).wait_send()

        @pl.when(core > 0)
        def _():
            y_copy(i).wait_send()
    for e in range(planes):
        for c in range(CORES):
            if e or c:
                own_copy(e, c, core).wait_send()

    @pl.when(core > 0)
    def _():
        own_copy(0, 0, core).wait_send()


def per_device(features, weights, sample_owner, sample_row, edge_src, edge_dst, edge_count):
    groups, shares = lax.axis_size("dp"), lax.axis_size("mp")
    kinds, feat, rows = features.shape
    sampled, edge_total = sample_row.shape[1], edge_src.shape[1]
    cap = 2 * sampled // groups
    items, planes = groups // CORES, shares // CORES
    width = weights.shape[2]
    quarter = width // shares
    bf16, f32, i32 = jnp.bfloat16, jnp.float32, jnp.int32
    vmem = pl.BlockSpec(memory_space=pltpu.VMEM)
    hbm = pl.BlockSpec(memory_space=pltpu.HBM)
    dma = pltpu.SemaphoreType.DMA
    return pl.pallas_call(
        functools.partial(kernel, groups, shares),
        out_shape=jax.ShapeDtypeStruct((kinds, quarter, SEEDS), bf16),
        in_specs=[hbm] * 7,
        out_specs=vmem,
        scratch_shapes=[
            pltpu.VMEM((kinds, 1, sampled), i32),
            pltpu.VMEM((kinds, sampled), i32),
            pltpu.VMEM(edge_src.shape, i32),
            pltpu.VMEM(edge_src.shape, i32),
            pltpu.SMEM((1, RELS), i32),
            pltpu.VMEM((kinds, CORES, feat, rows), bf16),
            pltpu.VMEM((CORES, MATS, feat, width), bf16),
            pltpu.VMEM((groups, kinds, cap + SEEDS), i32),
            pltpu.VMEM((items, kinds, cap + SEEDS), i32),
            pltpu.VMEM((SHARE, edge_total + SEEDS), i32),
            pltpu.VMEM((items, CORES, SHARE, edge_total + SEEDS), i32),
            pltpu.VMEM((kinds, 2 * sampled // LANES, LANES), bf16),
            pltpu.VMEM((16, edge_total), f32),
            pltpu.VMEM((16, edge_total), f32),
            pltpu.VMEM((2, kinds, cap, CORES * feat), bf16),
            pltpu.VMEM((MATS, SEEDS, cap), bf16),
            pltpu.VMEM((items, kinds, WAYS, planes, CORES, SEEDS // WAYS, quarter), bf16),
            pltpu.VMEM((items, kinds, WAYS, planes, CORES, SEEDS // WAYS, quarter), bf16),
            pltpu.VMEM((items, kinds, planes, CORES, SEEDS // WAYS, quarter), bf16),
            pltpu.VMEM((items, kinds, WAYS, CORES, SEEDS // WAYS, quarter), bf16),
            pltpu.VMEM((groups + (planes - 1) * (CORES + 1), kinds, WAYS, SEEDS // WAYS, quarter), bf16),
            dma((kinds + 1,)), dma((5,)), dma((kinds + 1,)), dma((kinds + 1,)),
            dma((items,)), dma((items,)),
            dma((groups,)), dma((items, CORES)),
            dma((items - 1, WAYS, planes - 1)), dma((items - 1, WAYS, planes - 1)),
            dma((items - 1,)), dma((items - 1,)),
            dma((items - 1, WAYS)), dma((groups, WAYS)),
            dma((planes, CORES)), dma((planes, CORES)),
            dma((planes, CORES)), dma((planes,)),
        ],
        compiler_params=pltpu.CompilerParams(
            collective_id=0, has_side_effects=True, vmem_limit_bytes=48 * 1024 * 1024),
    )(*[pltpu.with_memory_space_constraint(value, pltpu.HBM) for value in (
        features, weights, sample_owner.transpose(0, 2, 1), sample_row, edge_src, edge_dst, edge_count.T)])


def solution(mesh):
    return jax.shard_map(
        per_device,
        mesh=mesh,
        in_specs=(
            P(None, "mp", "dp"),
            P(None, "mp", None),
            P(None, "dp", None),
            P(None, "dp"),
            P(None, "dp"),
            P(None, "dp"),
            P(None, "dp"),
        ),
        out_specs=P(None, "mp", "dp"),
        check_vma=False,
    )
```

```python
import functools

import jax
import jax.numpy as jnp
from jax import lax
from jax.experimental import pallas as pl
from jax.experimental.pallas import tpu as pltpu
from jax.sharding import PartitionSpec as P

SEEDS = 128
RELATION_SOURCE = (0, 1, 0, 1, 2, 0, 2, 1)
MATRIX_TARGET = (1, 0, 0, 2, 1, 2, 0, 1, 0, 1, 2)
RELS = len(RELATION_SOURCE)
KINDS = 3
MATS = RELS + KINDS
SLOTS = tuple(
    tuple([r for r in range(RELS) if RELATION_SOURCE[r] == k] + [RELS + k]) for k in range(KINDS)
)
ORDER = tuple(m for group in SLOTS for m in group)
STARTS = tuple(sum(len(group) for group in SLOTS[:k]) for k in range(KINDS))
PLACE = tuple(ORDER.index(m) for m in range(MATS))
CORES = 2
WAYS = 2
SHARE = RELS // CORES
STEP = 256
LANES = 128
ONE_HOT = jnp.float8_e4m3fn
MESH = pl.DeviceIdType.MESH
NT = (((1,), (1,)), ((), ()))


def log2(n):
    return n.bit_length() - 1


def kernel(groups, shares, features_in, weights_in, owner_in, row_in, src_in, dst_in, count_in, out,
           owner, row, src, dst, count, feats, weights, req_send, req_recv, info_send, info_recv, table,
           lidx, ridx, picked, adj, xsend, xrecv, yrecv, zsend, zrecv,
           in_sem, list_sem, fx_ss, fx_rs, req_ss, req_rs, info_ss, info_rs, x_ss, x_rs, y_ss, y_rs, z_ss, z_rs, own_ss, own_rs, near_ss, near_rs):
    kinds, _, feat, rows = feats.shape
    both = CORES * feat
    sampled = row.shape[1]
    edge_total = src.shape[1]
    cap = req_send.shape[2] - SEEDS
    low = min(512, rows)
    high = rows // low
    lo_n = min(STEP, cap)
    hi_n = cap // lo_n
    items = groups // CORES
    planes = shares // CORES
    quarter = xsend.shape[6]
    span = SEEDS // WAYS
    half = CORES * quarter
    g = lax.axis_index("dp")
    m = lax.axis_index("mp")
    core = lax.rem(m, CORES)
    plane = m // CORES
    f32, bf16, i32 = jnp.float32, jnp.bfloat16, jnp.int32

    def at(group, mp):
        return {"dp": group, "mp": mp}

    def remote(source, target, ss, rs, group, mp):
        return pltpu.make_async_remote_copy(source, target, ss, rs, device_id=at(group, mp), device_id_type=MESH)

    def levels(size):
        return lax.broadcasted_iota(i32, (size, LANES), 0).astype(f32).astype(bf16)

    def hits(index, size, kind=bf16):
        level = levels(size)
        index = index.astype(f32).astype(bf16)
        yes, no = jnp.ones((), kind), jnp.zeros((), kind)
        return jnp.concatenate(
            [jnp.where(level == index[:, base:base + LANES], yes, no)
             for base in range(0, index.shape[1], LANES)], axis=1)

    mate = m - core + lax.rem(core + 1, CORES)
    loads, swaps = [], []
    for k in range(kinds):
        loads.append(pltpu.make_async_copy(features_in.at[k], feats.at[k, 0], in_sem.at[k]))
        swaps.append(remote(features_in.at[k], feats.at[k, 1], fx_ss.at[k], fx_rs.at[k], g, mate))
    loads.append(pltpu.make_async_copy(weights_in, weights.at[0], in_sem.at[kinds]))
    swaps.append(remote(weights_in, weights.at[1], fx_ss.at[kinds], fx_rs.at[kinds], g, mate))
    lists = [pltpu.make_async_copy(source, target, list_sem.at[n]) for n, (source, target) in enumerate(
        ((owner_in, owner), (row_in, row), (src_in, src), (dst_in, dst), (count_in, count)))]
    for copy in lists + loads:
        copy.start()

    barrier = pltpu.get_barrier_semaphore()
    pl.semaphore_signal(barrier, inc=1, device_id=at(g, mate), device_id_type=MESH)
    for d in range(1, groups):
        for c in range(CORES):
            pl.semaphore_signal(barrier, inc=1, device_id=at(g ^ d, plane * CORES + c), device_id_type=MESH)
    for e in range(1, planes):
        pl.semaphore_signal(
            barrier, inc=1, device_id=at(g, lax.rem(plane + e, planes) * CORES + core), device_id_type=MESH)
    pl.semaphore_wait(barrier, CORES * (groups - 1) + planes)
    for copy in swaps:
        copy.start()
    for copy in lists:
        copy.wait()

    tri = (lax.broadcasted_iota(i32, (STEP, STEP), 0) <= lax.broadcasted_iota(i32, (STEP, STEP), 1))
    tri = jnp.where(tri, 1.0, 0.0).astype(bf16)
    hot = jnp.concatenate([
        jnp.where(lax.broadcasted_iota(i32, (groups, sampled), 0) == owner[k], 1.0, 0.0)
        for k in range(kinds)], axis=0)
    lines = kinds * groups
    pieces = [hot[:, base:base + STEP] for base in range(0, sampled, STEP)]
    upto = jnp.dot(jnp.concatenate(pieces, axis=0).astype(bf16), tri, preferred_element_type=f32)
    carry = jnp.zeros((lines, 1), f32)
    ranks = []
    for n, piece in enumerate(pieces):
        here = upto[n * lines:(n + 1) * lines]
        ranks.append((here + (carry - 1.0)) * piece)
        carry = carry + here[:, STEP - 1:]
    ranks = jnp.concatenate(ranks, axis=1)

    blocks = sampled // LANES
    parts = cap // LANES
    places = []
    for k in range(kinds):
        mine = hot[k * groups:(k + 1) * groups]
        rank = jnp.sum(ranks[k * groups:(k + 1) * groups], axis=0, keepdims=True).astype(i32)
        places.append(owner[k] * cap + rank)
        wanted = row[k:k + 1, :]
        tall = mine * (wanted >> 8).astype(f32)
        wide = mine * (wanted & 255).astype(f32)
        bank = rank >> log2(LANES)
        stack = jnp.concatenate(
            [jnp.where(bank == h, part, 0.0) for part in (tall, wide) for h in range(parts)], axis=0).astype(bf16)
        listed = lax.dot_general(stack, hits(rank & (LANES - 1), LANES), NT, preferred_element_type=f32)
        listed = (listed[:parts * groups] * 256.0 + listed[parts * groups:]).astype(i32)
        seeds = jnp.where(mine[:, :SEEDS] > 0.0, rank[:, :SEEDS], -1)
        for o in range(groups):
            for h in range(parts):
                req_send[o, k:k + 1, h * LANES:(h + 1) * LANES] = listed[h * groups + o:h * groups + o + 1]
            req_send[o, k:k + 1, cap:] = seeds[o:o + 1]

    def order(i):
        return i + 2 if i < items - 2 else items - 1 - i

    def request_copy(t):
        to = g ^ (CORES * t + core)
        return remote(req_send.at[to], req_recv.at[t], req_ss.at[t], req_rs.at[t], to, m)

    for i in range(items):
        t = order(i)
        if t == 0:
            @pl.when(core > 0)
            def _():
                request_copy(0).start()

            @pl.when(core == 0)
            def _():
                req_recv[0] = req_send[g]
        else:
            request_copy(t).start()

    for k in range(kinds):
        coarse = (places[k] >> 8).astype(f32)
        fine = (places[k] & 255).astype(f32)
        table[k] = jnp.concatenate(
            [part[:, b * LANES:(b + 1) * LANES] for part in (coarse, fine) for b in range(blocks)], axis=0).astype(bf16)
    slots = lax.broadcasted_iota(i32, (1, edge_total), 1)
    banks = lax.broadcasted_iota(i32, (blocks, edge_total), 0)
    ones8 = jnp.ones((8, LANES), bf16)
    for j in range(SHARE):
        r = core * SHARE + j
        kind = RELATION_SOURCE[j] + core * (RELATION_SOURCE[SHARE + j] - RELATION_SOURCE[j])
        wanted = src[pl.ds(r, 1), :]
        found = jnp.dot(table[kind], hits(wanted & (LANES - 1), LANES), preferred_element_type=f32)
        found = found[:blocks] * 256.0 + found[blocks:]
        found = jnp.where(banks == (wanted >> log2(LANES)), found, 0.0)
        place = jnp.sum(found, axis=0, keepdims=True).astype(i32)
        live = slots < count[0, r]
        ends = dst[pl.ds(r, 1), :]
        info_send[j:j + 1, :edge_total] = jnp.where(live, place * SEEDS + ends, -1)
        marks = hits(jnp.where(live, ends, -1), SEEDS)
        tally = marks[:, :LANES]
        for base in range(LANES, edge_total, LANES):
            tally = tally + marks[:, base:base + LANES]
        tally = lax.dot_general(ones8, tally, NT, preferred_element_type=f32)
        info_send[j:j + 1, edge_total:] = tally[:1].astype(i32)

    def info_copy(d):
        return remote(info_send, info_recv.at[d // CORES, core], info_ss.at[d], info_rs.at[d // CORES, core],
                      g ^ d, plane * CORES + d % CORES)

    for i in range(items):
        for c in reversed(range(CORES)):
            d = CORES * order(i) + c
            if d == 0:
                @pl.when(core > 0)
                def _():
                    info_copy(0).start()

                @pl.when(core == 0)
                def _():
                    info_recv[0, 0] = info_send[...]
            else:
                info_copy(d).start()

    def info_wait(t, c):
        remote(info_send, info_recv.at[t, c], info_ss.at[0], info_rs.at[t, c], g, mate).wait_recv()

    def x_copy(i, w, e, t=slice(None)):
        to = lax.rem(plane + e, planes) * CORES + core
        return remote(xsend.at[i, t, w, e], xrecv.at[i, t, w, e], x_ss.at[i, w, e - 1], x_rs.at[i, w, e - 1], g, to)

    def y_copy(i, t=slice(None)):
        return remote(xsend.at[i, t, 1], yrecv.at[i, t], y_ss.at[i], y_rs.at[i], g ^ 1, plane * CORES)

    def z_copy(i, d, w, c, t):
        return remote(zsend.at[i, t, w, c], zrecv.at[d, t, w], z_ss.at[i, w], z_rs.at[d, w],
                      g ^ d, plane * CORES + c)

    near = items - 2

    def side(e):
        return CORES * order(near) if e == 0 else groups + (planes - 1) * CORES + e - 1

    def near_copy(e, c):
        return remote(xsend.at[near, :, 1, e, c], zrecv.at[side(e), :, 1], near_ss.at[e, c], near_rs.at[e],
                      g ^ (CORES * order(near)), lax.rem(plane + e, planes) * CORES + c)

    def z_sent(i, w):
        return remote(zsend.at[i, :, w], zsend.at[i, :, w], z_ss.at[i, w], z_rs.at[0, w], g, mate)

    def z_landed(d, w):
        return remote(zrecv.at[d, :, w], zrecv.at[d, :, w], z_ss.at[0, w], z_rs.at[d, w], g, mate)

    def far(e, d):
        return d if e == 0 else groups + (e - 1) * CORES + d

    def own_copy(e, c, d, t=slice(None)):
        return remote(xsend.at[items - 1, t, :, e, c], zrecv.at[far(e, d), t], own_ss.at[e, c], own_rs.at[e, d],
                      g ^ d, lax.rem(plane + e, planes) * CORES + c)

    def spot(i):
        return jnp.where(i < items - 2, i + 2, items - 1 - i)

    def merge(i):
        y_copy(i).wait_recv()
        for n in range(kinds):
            for e in range(planes):
                for c in range(CORES):
                    total = xsend[i, n, 1, e, c].astype(f32) + yrecv[i, n, e, c].astype(f32)
                    xsend[i, n, 1, e, c] = total.astype(bf16)
        for e in reversed(range(planes)):
            if isinstance(i, int) and i == near:
                for c in range(CORES):
                    near_copy(e, c).start()
            elif e:
                x_copy(i, 1, e).start()

    def deliver(i, w):
        d = CORES * spot(i) + core
        for e in range(1, planes):
            x_copy(i, w, e).wait_recv()
        for n in range(kinds):
            for c in range(CORES):
                total = xsend[i, n, w, 0, c].astype(f32)
                for e in range(1, planes):
                    total = total + xrecv[i, n, w, e, c].astype(f32)
                zsend[i, n, w, c] = total.astype(bf16)
        for c in range(CORES):
            z_copy(i, d, w, c, slice(None)).start()

    def pick(t, where, sides):
        tall = len(sides) * feat
        for k in range(kinds):
            wanted = req_recv[t, k:k + 1, :cap]
            bank = wanted >> log2(low)
            fine = wanted & (low - 1)
            choice = jnp.concatenate(
                [hits(jnp.where((fine >= base) & (fine < base + STEP), fine - base, -1), STEP)
                 for base in range(0, low, STEP)], axis=0)
            rows_k = jnp.concatenate(
                [feats[k, c, :, h * low:(h + 1) * low] for h in range(high) for c in sides], axis=0)
            found = jnp.dot(rows_k, choice, preferred_element_type=f32)
            chosen = found[:tall]
            for h in range(1, high):
                chosen = jnp.where(bank == h, found[h * tall:(h + 1) * tall], chosen)
            picked[where, k, :, sides[0] * feat:(sides[-1] + 1) * feat] = chosen.astype(bf16).T

    def build(place, ref_l, ref_r, n, width):
        left = hits(ref_l[n:n + 1, :width], lo_n, ONE_HOT)
        right = hits(ref_r[n:n + 1, :width], hi_n * SEEDS, ONE_HOT)
        counts = lax.dot_general(right, left, NT, preferred_element_type=f32).astype(bf16)
        for h in range(hi_n):
            adj[place, :, h * lo_n:(h + 1) * lo_n] = counts[h * SEEDS:(h + 1) * SEEDS]

    def item(i, first, last):
        t = order(i) if first or last else spot(i)
        where = 1 if last else 0
        if first:
            request_copy(t).wait_recv()
            pick(t, 0, range(CORES))
            for c in range(CORES):
                info_wait(t, c)
            loads[kinds].wait()
            swaps[kinds].wait()
        if not first and not last:
            pick(t, 0, range(CORES))
        for c in range(CORES):
            packed = info_recv[t, c, :, :edge_total] - g * (cap * SEEDS)
            ok = (packed >= 0) & (packed < cap * SEEDS)
            slot = packed >> log2(SEEDS)
            lidx[c * SHARE:(c + 1) * SHARE, :] = (slot & (lo_n - 1)).astype(f32)
            ridx[c * SHARE:(c + 1) * SHARE, :] = jnp.where(
                ok, (slot >> log2(lo_n)) * SEEDS + (packed & (SEEDS - 1)), -1).astype(f32)
        slot = req_recv[t, :, cap:]
        lidx[RELS:RELS + kinds, :SEEDS] = (slot & (lo_n - 1)).astype(f32)
        ridx[RELS:RELS + kinds, :SEEDS] = jnp.where(
            slot >= 0, (slot >> log2(lo_n)) * SEEDS + lax.broadcasted_iota(i32, slot.shape, 1), -1).astype(f32)
        degree = jnp.concatenate([info_recv[t, c, :, edge_total:] for c in range(CORES)], axis=0)
        inverse = (1.0 / jnp.maximum(degree.astype(f32), 1.0)).T
        groups_of = [[matrix for matrix in range(MATS) if MATRIX_TARGET[matrix] == n] for n in range(kinds)]

        def make(matrix):
            build(matrix, lidx, ridx, matrix, edge_total if matrix < RELS else SEEDS)

        def gather(n):
            values = []
            for matrix in groups_of[n]:
                kind = RELATION_SOURCE[matrix] if matrix < RELS else matrix - RELS
                value = jnp.dot(adj[matrix], picked[where, kind], preferred_element_type=f32)
                if matrix < RELS:
                    value = value * inverse[:, matrix:matrix + 1]
                values.append(value.astype(bf16))
            return jnp.concatenate(values, axis=1)

        def emit(n, left):
            right = jnp.concatenate([weights[c, matrix] for matrix in groups_of[n] for c in range(CORES)], axis=0)
            typed = jnp.dot(left, right, preferred_element_type=f32).astype(bf16)
            for p in range(planes):
                for w in range(WAYS):
                    for c in range(CORES):
                        xsend[i, n, w, lax.rem(p - plane + planes, planes), c] = typed[
                            w * span:(w + 1) * span, p * half + c * quarter:p * half + (c + 1) * quarter]
            if last:
                for e in reversed(range(planes)):
                    for c in range(CORES):
                        if e or c:
                            own_copy(e, c, core, n).start()

                @pl.when(core > 0)
                def _():
                    own_copy(0, 0, core, n).start()

                @pl.when(core == 0)
                def _():
                    for w in range(WAYS):
                        zrecv[0, n, w] = xsend[i, n, w, 0, 0]
            else:
                for e in range(1, planes):
                    x_copy(i, 0, e, n).start()

                @pl.when(core > 0)
                def _():
                    y_copy(i, n).start()

        for matrix in groups_of[0] + groups_of[1][:1]:
            make(matrix)
        left = gather(0)
        make(groups_of[1][1])
        emit(0, left)
        def relay():
            @pl.when((i >= 2) & (core == 0))
            def _():
                deliver(i - 2, 1)

        def advance():
            relay()

            @pl.when(core == 0)
            def _():
                merge(i - 1)

            deliver(i - 1, 0)

        if not first and not last:
            advance()
        for matrix in groups_of[1][2:] + groups_of[2][:1]:
            make(matrix)
        left = gather(1)
        for matrix in groups_of[2][1:]:
            make(matrix)
        emit(1, left)
        emit(2, gather(2))
        if last:
            advance()

    def rest(i, _):
        item(i, False, False)
        return 0

    for k in range(kinds):
        loads[k].wait()

    @pl.when(core > 0)
    def _():
        request_copy(0).wait_recv()
    pick(0, 1, (0,))
    for k in range(kinds):
        swaps[k].wait()
    pick(0, 1, (1,))
    item(0, True, False)
    for i in range(1, items - 1):
        request_copy(order(i)).wait_recv()
        for c in range(CORES):
            info_wait(order(i), c)
    info_wait(0, 1)

    @pl.when(core > 0)
    def _():
        info_wait(0, 0)
    lax.fori_loop(1, items - 1, rest, 0)
    item(items - 1, False, True)

    pieces = []
    for i in range(items - 1):
        for w in range(WAYS):
            for c in range(CORES if w == 0 else 1):
                d = CORES * order(i) + c
                if w == 0 or i < near:
                    z_landed(d, w).wait_recv()
                    pieces.append((w, d))
    for e in range(planes):
        near_copy(e, 0).wait_recv()
        pieces.append((1, side(e)))
    for e in range(planes):
        for d in range(CORES):
            if e or d:
                own_copy(e, 0, d).wait_recv()
            else:
                @pl.when(core > 0)
                def _():
                    own_copy(0, 0, 0).wait_recv()
            for w in range(WAYS):
                pieces.append((w, far(e, d)))
    for n in range(kinds):
        halves = []
        for w in range(WAYS):
            total = jnp.zeros((span, quarter), f32)
            for v, place in pieces:
                if v == w:
                    total = total + zrecv[place, n, w].astype(f32)
            halves.append(total)
        out[n] = jnp.maximum(jnp.concatenate(halves, axis=0), 0.0).T.astype(bf16)
    for t in range(items):
        if t == 0:
            @pl.when(core > 0)
            def _():
                request_copy(0).wait_send()
                info_copy(0).wait_send()
        else:
            request_copy(t).wait_send()
            info_copy(CORES * t).wait_send()
        for c in range(1, CORES):
            info_copy(CORES * t + c).wait_send()
    for i in range(items - 1):
        for e in range(1, planes):
            x_copy(i, 0, e).wait_send()
        z_sent(i, 0).wait_send()

        @pl.when(core == 0)
        def _():
            if i < near:
                for e in range(1, planes):
                    x_copy(i, 1, e).wait_send()
                z_sent(i, 1).wait_send()
            else:
                for e in range(planes):
                    for c in range(CORES):
                        near_copy(e, c).wait_send()

        @pl.when(core > 0)
        def _():
            y_copy(i).wait_send()
    for e in range(planes):
        for c in range(CORES):
            if e or c:
                own_copy(e, c, core).wait_send()

    @pl.when(core > 0)
    def _():
        own_copy(0, 0, core).wait_send()


def per_device(features, weights, sample_owner, sample_row, edge_src, edge_dst, edge_count):
    groups, shares = lax.axis_size("dp"), lax.axis_size("mp")
    kinds, feat, rows = features.shape
    sampled, edge_total = sample_row.shape[1], edge_src.shape[1]
    cap = 2 * sampled // groups
    items, planes = groups // CORES, shares // CORES
    width = weights.shape[2]
    quarter = width // shares
    bf16, f32, i32 = jnp.bfloat16, jnp.float32, jnp.int32
    vmem = pl.BlockSpec(memory_space=pltpu.VMEM)
    hbm = pl.BlockSpec(memory_space=pltpu.HBM)
    dma = pltpu.SemaphoreType.DMA
    return pl.pallas_call(
        functools.partial(kernel, groups, shares),
        out_shape=jax.ShapeDtypeStruct((kinds, quarter, SEEDS), bf16),
        in_specs=[hbm] * 7,
        out_specs=vmem,
        scratch_shapes=[
            pltpu.VMEM((kinds, 1, sampled), i32),
            pltpu.VMEM((kinds, sampled), i32),
            pltpu.VMEM(edge_src.shape, i32),
            pltpu.VMEM(edge_src.shape, i32),
            pltpu.SMEM((1, RELS), i32),
            pltpu.VMEM((kinds, CORES, feat, rows), bf16),
            pltpu.VMEM((CORES, MATS, feat, width), bf16),
            pltpu.VMEM((groups, kinds, cap + SEEDS), i32),
            pltpu.VMEM((items, kinds, cap + SEEDS), i32),
            pltpu.VMEM((SHARE, edge_total + SEEDS), i32),
            pltpu.VMEM((items, CORES, SHARE, edge_total + SEEDS), i32),
            pltpu.VMEM((kinds, 2 * sampled // LANES, LANES), bf16),
            pltpu.VMEM((16, edge_total), f32),
            pltpu.VMEM((16, edge_total), f32),
            pltpu.VMEM((2, kinds, cap, CORES * feat), bf16),
            pltpu.VMEM((MATS, SEEDS, cap), bf16),
            pltpu.VMEM((items, kinds, WAYS, planes, CORES, SEEDS // WAYS, quarter), bf16),
            pltpu.VMEM((items, kinds, WAYS, planes, CORES, SEEDS // WAYS, quarter), bf16),
            pltpu.VMEM((items, kinds, planes, CORES, SEEDS // WAYS, quarter), bf16),
            pltpu.VMEM((items, kinds, WAYS, CORES, SEEDS // WAYS, quarter), bf16),
            pltpu.VMEM((groups + (planes - 1) * (CORES + 1), kinds, WAYS, SEEDS // WAYS, quarter), bf16),
            dma((kinds + 1,)), dma((5,)), dma((kinds + 1,)), dma((kinds + 1,)),
            dma((items,)), dma((items,)),
            dma((groups,)), dma((items, CORES)),
            dma((items - 1, WAYS, planes - 1)), dma((items - 1, WAYS, planes - 1)),
            dma((items - 1,)), dma((items - 1,)),
            dma((items - 1, WAYS)), dma((groups, WAYS)),
            dma((planes, CORES)), dma((planes, CORES)),
            dma((planes, CORES)), dma((planes,)),
        ],
        compiler_params=pltpu.CompilerParams(
            collective_id=0, has_side_effects=True, vmem_limit_bytes=48 * 1024 * 1024),
    )(*[pltpu.with_memory_space_constraint(value, pltpu.HBM) for value in (
        features, weights, sample_owner.transpose(0, 2, 1), sample_row, edge_src, edge_dst, edge_count.T)])


def solution(mesh):
    return jax.shard_map(
        per_device,
        mesh=mesh,
        in_specs=(
            P(None, "mp", "dp"),
            P(None, "mp", None),
            P(None, "dp", None),
            P(None, "dp"),
            P(None, "dp"),
            P(None, "dp"),
            P(None, "dp"),
        ),
        out_specs=P(None, "mp", "dp"),
        check_vma=False,
    )
```
